32 devices in a mesh: grp: 4 (over y, core), mem: 8 (over z, x).
Axes of the slice: x: 2, y: 2, z: 4, core: 2. Of those that a mesh axis runs over, the one named last changes fastest.
Arguments:
- factors: bfloat16 [64, 288, 1792], P(('grp', 'mem')), may hold values from -1.5 to 1.5
- screen: int32 [32, 18], P(('grp', 'mem')), may hold values from 0 to 1, as said below
Outputs:
- exchange_matrix: float32 [1792, 1792], P(('grp', 'mem'))
The draws below stay inside these ranges and needn't reach their ends.
Inputs may be any that keep to these rules, and one draw needn't show every extreme that they name: screen[b, j] is 1 where auxiliary block b and occupied block j survive screening; every auxiliary block keeps at least one occupied block.
All inputs are finite; a program needn't handle non-finite values.
Results may differ from the reference program's by a relative error of at most 0.0003.
Values may be sent and summed in bfloat16 or wider, within the bound.
A program may use at most 128 MiB of HBM per device.

```python
import jax
import jax.numpy as jnp
from jax import lax

NBF = 1792
NOCC = 288
NOB = 18
NAB = 32
NAUX = 64


def draw_screen(key, part):
    count_key = jax.random.fold_in(key, 11)
    shuffle_key = jax.random.fold_in(key, 23)
    kept_count = jax.random.randint(count_key, (NAB, 1), 1, NOB + 1)
    row_keys = jax.random.split(shuffle_key, NAB)

    def shuffle_row(row_key):
        return jax.random.permutation(row_key, NOB)
    shuffled = jax.vmap(shuffle_row)(row_keys)
    position = jnp.argsort(shuffled, axis=1)
    return (position < kept_count).astype(jnp.int32)


def with_spikes(array, own_key, source, target, blocks, factor):
    def block_of(dim):
        return (jnp.arange(array.shape[dim]) // (array.shape[dim] // blocks)).reshape((-1,) + (1,) * (array.ndim - 1 - dim))

    near = jax.random.permutation(own_key, blocks)[block_of(target)]
    second = (block_of(target) + blocks // 2) % blocks
    return jnp.where((block_of(source) == near) | (block_of(source) == second), factor * array, array)


def steps_of(own_key, extent, pieces, low, top_value):
    def one(axis_at, parts):
        draws = jax.random.uniform(jax.random.fold_in(jax.random.fold_in(own_key, 6), axis_at), (parts,), jnp.float32, low / len(pieces), top_value / len(pieces))
        return jnp.repeat(jnp.exp(draws), extent[axis_at] // parts).reshape((-1,) + (1,) * (len(extent) - axis_at - 1))

    level = one(*pieces[0])
    for cut in pieces[1:]:
        level = level * one(*cut)
    return level


def bell_draw_with(own_key, dims, width, most, cuts, heavy, dtype=jnp.bfloat16):
    values = width * jax.random.normal(own_key, dims, jnp.float32)
    if cuts:
        values = values * steps_of(own_key, dims, cuts, -0.22, 0.18)
    return jnp.clip(with_spikes(values, jax.random.fold_in(own_key, 3), *heavy), -most, most).astype(dtype)


def setup_inputs(seed: int = 0) -> dict:
    keys = jax.random.split(jax.random.key(seed), 3)
    factors = bell_draw_with(keys[0], (NAUX, NOCC, NBF), 0.05, 1.5, ((0, 32),), (0, 2, 32, 2.75))
    screen = draw_screen(jax.random.fold_in(keys[2], 71), 0)
    return {"factors": factors, "screen": screen}


def reference(factors, screen):
    total_aux, occ_count, basis = factors.shape
    block_count, occ_blocks = screen.shape
    aux_rows = total_aux // block_count
    occ_width = occ_count // occ_blocks
    grouped = factors.reshape(block_count, aux_rows, occ_blocks, occ_width, basis)

    def add_block(running, pair):
        block, flags = pair
        masked = block * flags.astype(jnp.bfloat16)[None, :, None, None]
        flat_rows = masked.reshape(-1, basis)
        return running + jnp.dot(flat_rows.T, flat_rows, preferred_element_type=jnp.float32), None

    result, _ = lax.scan(add_block, jnp.zeros((basis, basis), jnp.float32), (grouped, screen))
    return result
```

```python
import functools

import jax
import jax.numpy as jnp
from jax import lax
from jax.experimental import pallas as pl
from jax.experimental.pallas import tpu as pltpu
from jax.sharding import PartitionSpec as P

LANES = 128
TOP = 32767.0
KINDS = "DGCFGFG"
STEPS = [0, 1, 2, 3, 4, 0, 1, 5, 6, 2, 3, 4, 0, 1, 5, 6]
MESH = pl.DeviceIdType.MESH


def bits_of(size):
    return size.bit_length() - 1


def plan_for(groups, members, parts):
    near = [[("mem", 1)]]
    rows = [[("grp", 2 << k)] for k in range(bits_of(groups) - 1)]
    far = [("mem", 2 << k) for k in range(bits_of(members) - 1)]
    single = [[bit] for bit in far]
    direct = [far[k : k + 2][::-1] for k in range(0, len(far), 2)]
    kinds = {
        "A": near + rows + direct,
        "B": rows + near + direct,
        "C": single + near + rows,
        "D": near + single + rows,
        "E": rows + single + near,
        "F": near + rows + single,
        "G": rows + near + single,
    }
    return [kinds[KINDS[p % len(KINDS)]] for p in range(parts)]


def messages_of(stages):
    left = 1
    for bits in stages:
        left <<= len(bits)
    result, slot = [], 0
    for level, bits in enumerate(stages):
        left >>= len(bits)
        for target in range(1, 1 << len(bits)):
            result.append((level, target, target * left, left, slot))
            slot += left
    return result


def kernel(
    groups, members, plan, chunks, width, x_ref, screen_ref, out_ref,
    both, turned, total, sent, got, sent_top, got_top, last,
    pair_send, pair_recv, data_send, data_recv, top_send, top_recv, end_send, end_recv,
):
    depth, basis = x_ref.shape
    own_rows = out_ref.shape[0]
    half = basis // 2
    occ_blocks = screen_ref.shape[1]
    grp, mem = lax.axis_index("grp"), lax.axis_index("mem")
    core = lax.rem(grp, 2)
    place = {"grp": grp, "mem": mem}
    def peer(bits):
        there = dict(place)
        for axis, step in bits:
            bit = lax.rem(place[axis] // step, 2)
            there[axis] = there[axis] + (1 - 2 * bit) * step
        return there["grp"], there["mem"]

    def chosen(bits, target):
        return tuple(b for t, b in enumerate(bits) if target >> (len(bits) - 1 - t) & 1)

    partner = peer([("grp", 1)])
    barrier = pltpu.get_barrier_semaphore()
    met = {
        tuple(sorted(chosen(stages[level], target)))
        for stages in plan
        for level, target, *_ in messages_of(stages)
    }
    peers = [partner] + [peer(bits) for bits in sorted(met)]
    for other in peers:
        pl.semaphore_signal(barrier, inc=1, device_id=other, device_id_type=MESH)


    def mask(j, carry):
        at = pl.ds(pl.multiple_of(j * width, width), width)
        keep = screen_ref[0, lax.rem(j, occ_blocks)].astype(jnp.float32)
        both[at, :] = (x_ref[at, :].astype(jnp.float32) * keep).astype(both.dtype)
        return carry

    pieces = 2
    piece = depth // pieces
    pair = []
    for n in range(pieces):
        lax.fori_loop(n * piece // width, (n + 1) * piece // width, mask, 0)
        if n == 0:
            pl.semaphore_wait(barrier, len(peers))
        pair.append(
            pltpu.make_async_remote_copy(
                src_ref=both.at[pl.ds(n * piece, piece)],
                dst_ref=both.at[pl.ds(depth + n * piece, piece)],
                send_sem=pair_send.at[n], recv_sem=pair_recv.at[n],
                device_id=partner, device_id_type=MESH,
            )
        )
        pair[-1].start()

    def turn(low, high):
        def one(m, carry):
            at = pl.ds(pl.multiple_of(m * 256, 256), 256)
            for k in range(low, high, LANES):
                turned[at, k : k + LANES] = both[k : k + LANES, at].T
            return carry

        lax.fori_loop(0, basis // 256, one, 0)

    early = depth // LANES * LANES
    turn(0, early)
    for copy in pair:
        copy.wait_recv()
    turn(early, 2 * depth)

    def rows_at(stages, index):
        order = [bit for bits in stages for bit in bits]
        at = {"grp": grp - core, "mem": mem}
        for t, (axis, step) in enumerate(order):
            flip = index // (1 << (len(order) - 1 - t)) % 2
            bit = lax.rem(place[axis] // step, 2)
            at[axis] = at[axis] + flip * (1 - 2 * bit) * step
        first = (at["grp"] * members + at["mem"]) * own_rows
        second = first + members * own_rows
        return [pl.ds(pl.multiple_of(r, 8), own_rows) for r in (first, second)]

    def repeat(low, high, body):
        count = high - low
        by = 4 if count % 4 == 0 else count

        def step(t, carry):
            for u in range(by):
                body(low + t * by + u)
            return carry

        if count == by:
            step(0, 0)
        else:
            lax.fori_loop(0, count // by, step, 0)

    def columns(p):
        return slice(p * LANES, (p + 1) * LANES)

    def current(p, index, order):
        return jnp.concatenate([total[r, columns(p)] for r in rows_at(order, index)], axis=0)

    def arrived(p, level, index):
        value = None
        for m, (at, _, _, _, slot) in enumerate(messages_of(plan[p])):
            if at == level:
                top = got_top[p, m, pl.ds(index, 1), :] * (1.0 / TOP)
                one = got[p, slot + index].astype(jnp.int32).astype(jnp.float32) * top
                value = one if value is None else value + one
        return value

    def copies(p, m):
        level, target, _, count, slot = messages_of(plan[p])[m]
        run = pl.ds(slot, count)
        to = peer(chosen(plan[p][level], target))
        return [
            pltpu.make_async_remote_copy(
                src_ref=here, dst_ref=there, send_sem=a.at[p, m], recv_sem=b.at[p, m],
                device_id=to, device_id_type=MESH,
            )
            for here, there, a, b in (
                (sent.at[p, run], got.at[p, run], data_send, data_recv),
                (sent_top.at[p, m], got_top.at[p, m], top_send, top_recv),
            )
        ]

    def send(p, level):
        for m, (at, _, first, count, slot) in reversed(list(enumerate(messages_of(plan[p])))):
            if at != level:
                continue

            def pack(i):
                value = current(p, first + i, plan[p])
                if level:
                    value = value + arrived(p, level - 1, first + i)
                top = jnp.max(jnp.abs(value), axis=0, keepdims=True)
                scale = TOP / jnp.maximum(top, 2e-34)
                sent[p, slot + i] = jnp.round(value * scale).astype(jnp.int32).astype(jnp.int16)
                sent_top[p, m, pl.ds(i, 1), :] = top

            repeat(0, count, pack)
            for copy in copies(p, m):
                copy.start()

    def wait(p, level):
        for m, (at, *_) in enumerate(messages_of(plan[p])):
            if at == level:
                for copy in copies(p, m):
                    copy.wait_recv()

    def keep(p, level):
        count = [n for at, _, _, n, _ in messages_of(plan[p]) if at == level][0]
        if level + 1 < len(plan[p]):
            count >>= len(plan[p][level + 1])

        def add(i):
            value = arrived(p, level, i)
            for n, r in enumerate(rows_at(plan[p], i)):
                total[r, columns(p)] += value[n * own_rows : (n + 1) * own_rows]

        repeat(0, count, add)

    parts = len(plan)
    mine = pl.ds(pl.multiple_of((grp * members + mem) * own_rows, 8), own_rows)
    theirs = pl.ds(pl.multiple_of((partner[0] * members + mem) * own_rows, 8), own_rows)
    ends = []

    def advance(p, level):
        wait(p, level)
        if level + 1 < len(plan[p]):
            send(p, level + 1)
            keep(p, level)
            return
        keep(p, level)
        last[p] = total[theirs, columns(p)]
        at = pl.ds(pl.multiple_of(core * half + p * LANES, LANES), LANES)
        copy = pltpu.make_async_remote_copy(
            src_ref=last.at[p], dst_ref=out_ref.at[:, at],
            send_sem=end_send.at[p], recv_sem=end_recv.at[p],
            device_id=partner, device_id_type=MESH,
        )
        copy.start()
        ends.append(copy)
        out_ref[:, at] = total[mine, columns(p)]

    def multiply(low, high):
        def one(m, carry):
            tall = basis // 2
            at = pl.ds(pl.multiple_of(m * tall, LANES), tall)
            total[at, low:high] = jnp.dot(
                turned[at, :],
                both[:, pl.ds(pl.multiple_of(core * half + low, LANES), high - low)],
                preferred_element_type=jnp.float32,
            )
            return carry

        lax.fori_loop(0, 2, one, 0)

    step = [0] * parts
    made = 0
    for p in STEPS + list(range(parts)) * (2 + max(len(stages) for stages in plan)):
        if p >= parts or step[p] > len(plan[p]):
            continue
        if step[p] == 0:
            while chunks[made][0] <= p * LANES if made < len(chunks) else False:
                multiply(*chunks[made])
                made += 1
            send(p, 0)
        else:
            advance(p, step[p] - 1)
        step[p] += 1
    for copy in pair:
        copy.wait_send()
    for p in range(parts):
        for m in range(len(messages_of(plan[p]))):
            for copy in copies(p, m):
                copy.wait_send()
    for copy in ends:
        copy.wait()


NEAR, ROW = ("mem", 1), ("grp", 2)
ORDERS = ["xyab", "ayxb", "yabx", "yxab"]
STEPS_AFTER = [0, 0, 2, 1, 3, 2, 0, 1, 3, 2, 0, 1, 3, 2, 1, 3]


def circle_plan(groups, members, parts):
    far = [("mem", 2 << k) for k in range(bits_of(members) - 1)]
    letters = {
        "x": [[NEAR]],
        "y": [[("grp", 2 << k)] for k in range(bits_of(groups) - 1)],
        "a": [far[:1]],
        "b": [[bit] for bit in far[1:]],
        "z": [far[::-1]],
    }
    orders = [ORDERS[p % len(ORDERS)] for p in range(parts)]
    return [[stage for letter in order for stage in letters[letter]] for order in orders]


def place_of(groups, members, at):
    ladder, line = groups // 2, members // 2
    w, z = at // line, at % line
    z = line - 1 - z if w % 2 else z
    return (w, z, 0) if w < ladder else (2 * ladder - 1 - w, z, 1)


def moves_of(groups, members, own_rows, basis):
    unit = 2 * own_rows
    moves = []
    for low in range(0, basis, LANES):
        pieces, c = [], low
        while c < low + LANES:
            y, z, x = place_of(groups, members, c // unit)
            half, off = c % unit // own_rows, c % own_rows
            source = ((2 * y + half) * members + 2 * z + x) * own_rows + off
            count = min(own_rows - off, low + LANES - c, LANES - source % LANES)
            pieces.append((c - low, source // LANES, (c - low - source) % LANES))
            c += count
        moves.append(pieces)
    return moves


def circle_kernel(
    groups, members, plan, width, x_hbm, screen_ref, out_ref,
    x_ref, both, turned, total, sent, got, sent_top, got_top, last, window, flipped, around,
    load, pair_send, pair_recv, data_send, data_recv, top_send, top_recv, end_send, end_recv,
    flip_send, flip_recv,
):
    depth, basis = x_ref.shape
    own_rows = out_ref.shape[0]
    pieces = pair_send.shape[0]
    piece = depth // pieces
    loads = []
    for n in range(pieces):
        at = pl.ds(n * piece, piece)
        loads.append(pltpu.make_async_copy(x_hbm.at[at], x_ref.at[at], load.at[n]))
        loads[-1].start()
    unit = 2 * own_rows
    chips = groups * members // 2
    line, ladder = members // 2, groups // 2
    reach = chips // 2
    parts = len(plan)
    panels = basis // LANES
    occ_blocks = screen_ref.shape[1]
    grp, mem = lax.axis_index("grp"), lax.axis_index("mem")
    core = lax.rem(grp, 2)
    place = {"grp": grp - core, "mem": mem}
    lane = lax.broadcasted_iota(jnp.int32, (1, LANES), 1)
    swap = {NEAR: ROW, ROW: NEAR}

    def step_of(bit):
        axis, step = bit
        return step * (1 - 2 * lax.rem(place[axis] // step, 2))

    def moved(bits):
        there = dict(place)
        for bit in bits:
            other = swap.get(bit, bit)
            if other == bit:
                there[bit[0]] = there[bit[0]] + step_of(bit)
            else:
                there[bit[0]] = there[bit[0]] + step_of(bit) * (1 - core)
                there[other[0]] = there[other[0]] + step_of(other) * core
        return there["grp"], there["mem"]

    def peer(bits):
        g, m = moved(bits)
        return g + core, m

    def spot(g, m):
        y, z, x = g // 2, m // 2, lax.rem(m, 2)
        w = jnp.where(x == 1, 2 * ladder - 1 - y, y)
        return w * line + jnp.where(lax.rem(w, 2) == 1, line - 1 - z, z)

    def holder(at):
        w, z = at // line, lax.rem(at, line)
        z = jnp.where(lax.rem(w, 2) == 1, line - 1 - z, z)
        x = jnp.where(w >= ladder, 1, 0)
        y = jnp.where(w >= ladder, 2 * ladder - 1 - w, w)
        return 2 * y, 2 * z + x

    def chosen(bits, target):
        return tuple(b for t, b in enumerate(bits) if target >> (len(bits) - 1 - t) & 1)

    own = spot(grp, mem)
    partner = (grp + 1 - 2 * core, mem)
    barrier = pltpu.get_barrier_semaphore()
    met = {
        tuple(sorted(chosen(stages[level], target)))
        for stages in plan
        for level, target, *_ in messages_of(stages)
    }
    met |= {tuple(sorted(swap.get(b, b) for b in bits)) for bits in met}
    peers = [partner] + [peer(bits) for bits in sorted(met)]
    for other in peers:
        pl.semaphore_signal(barrier, inc=1, device_id=other, device_id_type=MESH)

    moves = moves_of(groups, members, own_rows, basis)

    def arrange(j, carry):
        for u in range(strips):
            row = j * strips + u
            at = pl.ds(pl.multiple_of(row * width, width), width)
            keep = screen_ref[0, lax.rem(row, occ_blocks)].astype(jnp.float32).astype(both.dtype)
            for n, pieces in enumerate(moves):
                value = None
                for first, m, shift in pieces:
                    piece = x_ref[at, columns(m)]
                    piece = pltpu.roll(piece, shift, 1) if shift else piece
                    value = piece if value is None else jnp.where(lane >= first, piece, value)
                value = value * keep
                both[at, columns(n)] = value
                if n == 0:
                    both[at, columns(panels)] = value
        return carry

    def columns(p):
        return slice(p * LANES, (p + 1) * LANES)

    strips = 3
    pair = []
    for n in range(pieces):
        with jax.named_scope(f"load{n}"):
            loads[n].wait()
        with jax.named_scope(f"arrange{n}"):
            count = piece // width // strips
            lax.fori_loop(n * count, (n + 1) * count, arrange, 0)
        if n == 0:
            with jax.named_scope("barrier"):
                pl.semaphore_wait(barrier, len(peers))
        pair.append(
            pltpu.make_async_remote_copy(
                src_ref=both.at[pl.ds(n * piece, piece)],
                dst_ref=both.at[pl.ds(depth + n * piece, piece)],
                send_sem=pair_send.at[n], recv_sem=pair_recv.at[n],
                device_id=partner, device_id_type=MESH,
            )
        )
        pair[-1].start()

    def turn(low, high):
        def one(m, carry):
            at = pl.ds(pl.multiple_of(m * wide, LANES), wide)
            for k in range(low, high, LANES):
                turned[at, k : k + LANES] = both[k : k + LANES, at].T
            return carry

        wide = basis // 2
        lax.fori_loop(0, 2, one, 0)

    early = depth // LANES * LANES
    with jax.named_scope("turn"):
        turn(0, early)
    done = 0
    for low in range(early, 2 * depth, LANES):
        while done < pieces and low + LANES > depth + done * piece:
            with jax.named_scope(f"pair{done}"):
                pair[done].wait_recv()
            done += 1
        with jax.named_scope(f"turn{low}"):
            turn(low, low + LANES)

    def rows_of(stages, index):
        order = [bit for bits in stages for bit in bits]
        flips = [b for t, b in enumerate(order) if False]
        there = dict(place)
        for t, bit in enumerate(order):
            flip = index // (1 << (len(order) - 1 - t)) % 2
            other = swap.get(bit, bit)
            if other == bit:
                there[bit[0]] = there[bit[0]] + flip * step_of(bit)
            else:
                there[bit[0]] = there[bit[0]] + flip * step_of(bit) * (1 - core)
                there[other[0]] = there[other[0]] + flip * step_of(other) * core
        return spot(there["grp"], there["mem"])

    def repeat(low, high, body):
        count = high - low
        by = 8 if count % 8 == 0 else count

        def step(t, carry):
            for u in range(by):
                body(low + t * by + u)
            return carry

        if count == by:
            step(0, 0)
        else:
            lax.fori_loop(0, count // by, step, 0)

    def panel_of(p):
        return jnp.where(core == 0, parts - 1 - p, parts + p)

    def block_at(s):
        return pl.ds(pl.multiple_of(s * unit, 16), unit)

    def product(p, s):
        start = s * unit + panel_of(p) * LANES
        start = jnp.where(start >= basis, start - basis, start)
        n = start // LANES
        a = start - n * LANES
        value = jnp.dot(
            turned[block_at(s), :],
            both[:, pl.ds(pl.multiple_of(n * LANES, LANES), 2 * LANES)],
            preferred_element_type=jnp.float32,
        )
        value = jnp.where(lane >= a, value[:, :LANES], value[:, LANES:])
        return pltpu.roll(value, jnp.where(a == 0, 0, LANES - a), 1)

    def current(p, index):
        return total[block_at(rows_of(plan[p], index)), columns(p)]

    def arrived(p, level, index):
        value = None
        for m, (at, _, _, _, slot) in enumerate(messages_of(plan[p])):
            if at == level:
                top = got_top[p, m, pl.ds(index, 1), :] * (1.0 / TOP)
                one = got[p, slot + index].astype(jnp.int32).astype(jnp.float32) * top
                value = one if value is None else value + one
        return value

    def copies(p, m):
        level, target, _, count, slot = messages_of(plan[p])[m]
        run = pl.ds(slot, count)
        to = peer(chosen(plan[p][level], target))
        return [
            pltpu.make_async_remote_copy(
                src_ref=here, dst_ref=there, send_sem=a.at[p, m], recv_sem=b.at[p, m],
                device_id=to, device_id_type=MESH,
            )
            for here, there, a, b in (
                (sent.at[p, run], got.at[p, run], data_send, data_recv),
                (sent_top.at[p, m], got_top.at[p, m], top_send, top_recv),
            )
        ]

    def send(p, level):
        for m, (at, _, first, count, slot) in reversed(list(enumerate(messages_of(plan[p])))):
            if at != level:
                continue

            def pack(i):
                if level:
                    value = current(p, first + i) + arrived(p, level - 1, first + i)
                else:
                    value = product(p, rows_of(plan[p], first + i))
                top = jnp.max(jnp.abs(value), axis=0, keepdims=True)
                scale = TOP / jnp.maximum(top, 2e-34)
                sent[p, slot + i] = jnp.round(value * scale).astype(jnp.int32).astype(jnp.int16)
                sent_top[p, m, pl.ds(i, 1), :] = top

            repeat(0, count, pack)
            for copy in copies(p, m):
                copy.start()

    def remaining(p, level):
        count = [n for at, _, _, n, _ in messages_of(plan[p]) if at == level][0]
        return count

    def fill(p):
        def one(i):
            s = rows_of(plan[p], i)
            total[block_at(s), columns(p)] = product(p, s)

        repeat(0, remaining(p, 0), one)

    def wait(p, level):
        for m, (at, *_) in enumerate(messages_of(plan[p])):
            if at == level:
                for copy in copies(p, m):
                    copy.wait_recv()

    def keep(p, level):
        count = remaining(p, level)
        if level + 1 < len(plan[p]):
            count >>= len(plan[p][level + 1])

        def add(i):
            total[block_at(rows_of(plan[p], i)), columns(p)] += arrived(p, level, i)

        repeat(0, count, add)

    def cuts(p, side):
        q = parts - 1 - p if side == 0 else parts + p
        marks = sorted({q * LANES, (q + 1) * LANES} | {
            r for r in range(q * LANES, (q + 1) * LANES) if r % own_rows == 0
        })
        result = []
        for t, (low, high) in enumerate(zip(marks, marks[1:])):
            k, half = low // unit, low % unit // own_rows
            if 0 < k < reach:
                result.append((q, t, k, half, low - q * LANES, low % own_rows, high - low))
        return result

    def flips(p, side):
        result = []
        for q, t, k, half, here, there, count in cuts(p, side):
            g, m = holder(lax.rem(own + k, chips))
            copy = pltpu.make_async_remote_copy(
                src_ref=flipped.at[p, pl.ds(here, count)],
                dst_ref=around.at[chips - k, pl.ds(there, count)],
                send_sem=flip_send.at[p, t], recv_sem=flip_recv.at[q, t],
                device_id=(g + half, m), device_id_type=MESH,
            )
            result.append((half, copy))
        return result

    def ends(p):
        q = panel_of(p)
        at = pl.ds(pl.multiple_of(q * LANES, LANES), LANES)
        return pltpu.make_async_remote_copy(
            src_ref=last.at[p], dst_ref=window.at[:, at],
            send_sem=end_send.at[p], recv_sem=end_recv.at[p],
            device_id=partner, device_id_type=MESH,
        )

    def finish(p):
        mine = pl.ds(pl.multiple_of(own * unit + core * own_rows, 8), own_rows)
        theirs = pl.ds(pl.multiple_of(own * unit + (1 - core) * own_rows, 8), own_rows)
        value = total[block_at(own), columns(p)]
        flipped[p, :, :unit] = value.T
        for side in range(2):
            if cuts(p, side):
                @pl.when(core == side)
                def _():
                    for _, copy in flips(p, side):
                        copy.start()
        last[p] = total[theirs, columns(p)]
        ends(p).start()
        at = pl.ds(pl.multiple_of(panel_of(p) * LANES, LANES), LANES)
        window[:, at] = total[mine, columns(p)]

    for p in range(parts):
        with jax.named_scope(f"send{p}_0"):
            send(p, 0)
    for copy in pair:
        copy.wait_send()
    level = [0] * parts
    for p in STEPS_AFTER + list(range(parts)) * 8:
        if p >= parts or level[p] >= len(plan[p]):
            continue
        if level[p] == 0:
            with jax.named_scope(f"fill{p}"):
                fill(p)
        with jax.named_scope(f"wait{p}_{level[p]}"):
            wait(p, level[p])
        if level[p] + 1 < len(plan[p]):
            with jax.named_scope(f"send{p}_{level[p] + 1}"):
                send(p, level[p] + 1)
        with jax.named_scope(f"keep{p}_{level[p]}"):
            keep(p, level[p])
        with jax.named_scope(f"sent{p}_{level[p]}"):
            for m, (at, *_) in enumerate(messages_of(plan[p])):
                if at == level[p]:
                    for copy in copies(p, m):
                        copy.wait_send()
        level[p] += 1
        if level[p] == len(plan[p]):
            with jax.named_scope(f"finish{p}"):
                finish(p)

    with jax.named_scope("ends"):
        for p in range(parts):
            ends(p).wait_recv()
    for k in range(reach + 1):
        n, a = k * unit // LANES, k * unit % LANES
        value = window[:, columns(n)]
        if a:
            if a + unit > LANES:
                value = jnp.where(lane >= a, value, window[:, columns(n + 1)])
            value = pltpu.roll(value, LANES - a, 1)
        around[k] = value
    with jax.named_scope("flips"):
      for side in range(2):
        @pl.when(core == side)
        def _():
            for p in range(parts):
                for origin in range(2):
                    for half, copy in flips(p, origin):
                        if half == side:
                            copy.wait_recv()

    with jax.named_scope("out"):
      for n in range(panels):
        value, c = None, n * LANES
        while c < (n + 1) * LANES:
            b, off = c // own_rows, c % own_rows
            g, m = b // members, b % members
            z, x, y = m // 2, m % 2, g // 2
            w = 2 * ladder - 1 - y if x else y
            s = w * line + (line - 1 - z if w % 2 else z)
            piece = around[lax.rem(s - own + chips, chips)]
            shift = (c - n * LANES - (g % 2 * own_rows + off)) % LANES
            piece = pltpu.roll(piece, shift, 1) if shift else piece
            value = piece if value is None else jnp.where(lane >= c - n * LANES, piece, value)
            c += min(own_rows - off, (n + 1) * LANES - c)
        out_ref[:, columns(n)] = value

    with jax.named_scope("last"):
     for p in range(parts):
        ends(p).wait_send()
        for side in range(2):
            if cuts(p, side):
                @pl.when(core == side)
                def _():
                    for _, copy in flips(p, side):
                        copy.wait_send()


def circle_call(groups, members, rows, screen, own_rows, width):
    depth, basis = rows.shape
    unit = 2 * own_rows
    chips = groups * members // 2
    parts = -(-(chips // 2 + 1) * unit // LANES) // 2
    plan = circle_plan(groups, members, parts)
    levels = max(len(messages_of(stages)) for stages in plan)
    places = max(8, chips // 2)
    pieces = 4
    dma = pltpu.SemaphoreType.DMA
    vmem = pl.BlockSpec(memory_space=pltpu.VMEM)
    return pl.pallas_call(
        functools.partial(circle_kernel, groups, members, plan, width),
        out_shape=pltpu.VMEM((own_rows, basis), jnp.float32),
        in_specs=[pl.BlockSpec(memory_space=pl.ANY), pl.BlockSpec(memory_space=pltpu.SMEM)],
        out_specs=vmem,
        scratch_shapes=[
            pltpu.VMEM((depth, basis), jnp.bfloat16),
            pltpu.VMEM((2 * depth, basis + LANES), jnp.bfloat16),
            pltpu.VMEM((basis, 2 * depth), jnp.bfloat16),
            pltpu.VMEM((basis, parts * LANES), jnp.float32),
            pltpu.VMEM((parts, chips - 1, unit, LANES), jnp.int16),
            pltpu.VMEM((parts, chips - 1, unit, LANES), jnp.int16),
            pltpu.VMEM((parts, levels, places, LANES), jnp.float32),
            pltpu.VMEM((parts, levels, places, LANES), jnp.float32),
            pltpu.VMEM((parts, own_rows, LANES), jnp.float32),
            pltpu.VMEM((own_rows, 2 * parts * LANES), jnp.float32),
            pltpu.VMEM((parts, LANES, LANES), jnp.float32),
            pltpu.VMEM((chips, own_rows, LANES), jnp.float32),
            dma((pieces,)), dma((pieces,)), dma((pieces,)),
            dma((parts, levels)), dma((parts, levels)),
            dma((parts, levels)), dma((parts, levels)),
            dma((parts,)), dma((parts,)),
            dma((parts, 8)), dma((2 * parts, 8)),
        ],
        compiler_params=pltpu.CompilerParams(
            collective_id=1, has_side_effects=True, vmem_limit_bytes=60 * 1024 * 1024
        ),
    )(rows, screen)


def circle_fits(groups, members, own_rows, basis, depth, width):
    unit = 2 * own_rows
    chips = groups * members // 2
    panels = -(-(chips // 2 + 1) * unit // LANES)
    return (
        groups >= 4 and members >= 4 and 64 < unit <= LANES and unit % 16 == 0
        and basis % 256 == 0 and panels % 2 == 0 and depth % (4 * width) == 0
    )


def solution(mesh):
    groups, members = mesh.shape["grp"], mesh.shape["mem"]

    def on_device(factors, screen):
        aux_rows, occ_count, basis = factors.shape
        depth = aux_rows * occ_count
        devices = groups * members
        real_rows = basis // devices
        own_rows = (real_rows + 7) // 8 * 8
        rows = factors.reshape(depth, basis)
        if own_rows != real_rows:
            rows = rows.reshape(depth, devices, real_rows)
            rows = jnp.pad(rows, ((0, 0), (0, 0), (0, own_rows - real_rows)))
            basis = devices * own_rows
            rows = rows.reshape(depth, basis)
        width = occ_count // screen.shape[1]
        if own_rows == real_rows and circle_fits(groups, members, own_rows, basis, depth, width):
            return circle_call(groups, members, rows, screen, own_rows, width)
        half = basis // 2
        parts = half // LANES
        plan = plan_for(groups, members, parts)
        chunks = [(low, min(low + 2 * LANES, half)) for low in range(0, half, 2 * LANES)]
        chips = groups * members // 2
        levels = max(len(messages_of(stages)) for stages in plan)
        block = 2 * own_rows
        places = max(8, chips // 2)
        dma = pltpu.SemaphoreType.DMA
        vmem = pl.BlockSpec(memory_space=pltpu.VMEM)
        result = pl.pallas_call(
            functools.partial(kernel, groups, members, plan, chunks, occ_count // screen.shape[1]),
            out_shape=pltpu.VMEM((own_rows, basis), jnp.float32),
            in_specs=[vmem, pl.BlockSpec(memory_space=pltpu.SMEM)],
            out_specs=vmem,
            scratch_shapes=[
                pltpu.VMEM((2 * depth, basis), jnp.bfloat16),
                pltpu.VMEM((basis, 2 * depth), jnp.bfloat16),
                pltpu.VMEM((basis, half), jnp.float32),
                pltpu.VMEM((parts, chips - 1, block, LANES), jnp.int16),
                pltpu.VMEM((parts, chips - 1, block, LANES), jnp.int16),
                pltpu.VMEM((parts, levels, places, LANES), jnp.float32),
                pltpu.VMEM((parts, levels, places, LANES), jnp.float32),
                pltpu.VMEM((parts, own_rows, LANES), jnp.float32),
                dma((2,)), dma((2,)),
                dma((parts, levels)), dma((parts, levels)),
                dma((parts, levels)), dma((parts, levels)),
                dma((parts,)), dma((parts,)),
            ],
            compiler_params=pltpu.CompilerParams(
                collective_id=0, has_side_effects=True, vmem_limit_bytes=60 * 1024 * 1024
            ),
        )(rows, screen)
        if own_rows != real_rows:
            result = result[:real_rows].reshape(real_rows, devices, own_rows)[:, :, :real_rows]
            result = result.reshape(real_rows, devices * real_rows)
        return result

    placed = (P(("grp", "mem"), None, None), P(("grp", "mem"), None))
    return jax.shard_map(
        on_device, mesh=mesh, in_specs=placed, out_specs=P(("grp", "mem"), None), check_vma=False
    )
```

```python
import functools

import jax
import jax.numpy as jnp
from jax import lax
from jax.experimental import pallas as pl
from jax.experimental.pallas import tpu as pltpu
from jax.sharding import PartitionSpec as P

LANES = 128
TOP = 32767.0
KINDS = "DGCFGFG"
STEPS = [0, 1, 2, 3, 4, 0, 1, 5, 6, 2, 3, 4, 0, 1, 5, 6]
MESH = pl.DeviceIdType.MESH


def bits_of(size):
    return size.bit_length() - 1


def plan_for(groups, members, parts):
    near = [[("mem", 1)]]
    rows = [[("grp", 2 << k)] for k in range(bits_of(groups) - 1)]
    far = [("mem", 2 << k) for k in range(bits_of(members) - 1)]
    single = [[bit] for bit in far]
    direct = [far[k : k + 2][::-1] for k in range(0, len(far), 2)]
    kinds = {
        "A": near + rows + direct,
        "B": rows + near + direct,
        "C": single + near + rows,
        "D": near + single + rows,
        "E": rows + single + near,
        "F": near + rows + single,
        "G": rows + near + single,
    }
    return [kinds[KINDS[p % len(KINDS)]] for p in range(parts)]


def messages_of(stages):
    left = 1
    for bits in stages:
        left <<= len(bits)
    result, slot = [], 0
    for level, bits in enumerate(stages):
        left >>= len(bits)
        for target in range(1, 1 << len(bits)):
            result.append((level, target, target * left, left, slot))
            slot += left
    return result


def kernel(
    groups, members, plan, chunks, width, x_ref, screen_ref, out_ref,
    both, turned, total, sent, got, sent_top, got_top, last,
    pair_send, pair_recv, data_send, data_recv, top_send, top_recv, end_send, end_recv,
):
    depth, basis = x_ref.shape
    own_rows = out_ref.shape[0]
    half = basis // 2
    occ_blocks = screen_ref.shape[1]
    grp, mem = lax.axis_index("grp"), lax.axis_index("mem")
    core = lax.rem(grp, 2)
    place = {"grp": grp, "mem": mem}
    def peer(bits):
        there = dict(place)
        for axis, step in bits:
            bit = lax.rem(place[axis] // step, 2)
            there[axis] = there[axis] + (1 - 2 * bit) * step
        return there["grp"], there["mem"]

    def chosen(bits, target):
        return tuple(b for t, b in enumerate(bits) if target >> (len(bits) - 1 - t) & 1)

    partner = peer([("grp", 1)])
    barrier = pltpu.get_barrier_semaphore()
    met = {
        tuple(sorted(chosen(stages[level], target)))
        for stages in plan
        for level, target, *_ in messages_of(stages)
    }
    peers = [partner] + [peer(bits) for bits in sorted(met)]
    for other in peers:
        pl.semaphore_signal(barrier, inc=1, device_id=other, device_id_type=MESH)


    def mask(j, carry):
        at = pl.ds(pl.multiple_of(j * width, width), width)
        keep = screen_ref[0, lax.rem(j, occ_blocks)].astype(jnp.float32)
        both[at, :] = (x_ref[at, :].astype(jnp.float32) * keep).astype(both.dtype)
        return carry

    pieces = 2
    piece = depth // pieces
    pair = []
    for n in range(pieces):
        lax.fori_loop(n * piece // width, (n + 1) * piece // width, mask, 0)
        if n == 0:
            pl.semaphore_wait(barrier, len(peers))
        pair.append(
            pltpu.make_async_remote_copy(
                src_ref=both.at[pl.ds(n * piece, piece)],
                dst_ref=both.at[pl.ds(depth + n * piece, piece)],
                send_sem=pair_send.at[n], recv_sem=pair_recv.at[n],
                device_id=partner, device_id_type=MESH,
            )
        )
        pair[-1].start()

    def turn(low, high):
        def one(m, carry):
            at = pl.ds(pl.multiple_of(m * 256, 256), 256)
            for k in range(low, high, LANES):
                turned[at, k : k + LANES] = both[k : k + LANES, at].T
            return carry

        lax.fori_loop(0, basis // 256, one, 0)

    early = depth // LANES * LANES
    turn(0, early)
    for copy in pair:
        copy.wait_recv()
    turn(early, 2 * depth)

    def rows_at(stages, index):
        order = [bit for bits in stages for bit in bits]
        at = {"grp": grp - core, "mem": mem}
        for t, (axis, step) in enumerate(order):
            flip = index // (1 << (len(order) - 1 - t)) % 2
            bit = lax.rem(place[axis] // step, 2)
            at[axis] = at[axis] + flip * (1 - 2 * bit) * step
        first = (at["grp"] * members + at["mem"]) * own_rows
        second = first + members * own_rows
        return [pl.ds(pl.multiple_of(r, 8), own_rows) for r in (first, second)]

    def repeat(low, high, body):
        count = high - low
        by = 4 if count % 4 == 0 else count

        def step(t, carry):
            for u in range(by):
                body(low + t * by + u)
            return carry

        if count == by:
            step(0, 0)
        else:
            lax.fori_loop(0, count // by, step, 0)

    def columns(p):
        return slice(p * LANES, (p + 1) * LANES)

    def current(p, index, order):
        return jnp.concatenate([total[r, columns(p)] for r in rows_at(order, index)], axis=0)

    def arrived(p, level, index):
        value = None
        for m, (at, _, _, _, slot) in enumerate(messages_of(plan[p])):
            if at == level:
                top = got_top[p, m, pl.ds(index, 1), :] * (1.0 / TOP)
                one = got[p, slot + index].astype(jnp.int32).astype(jnp.float32) * top
                value = one if value is None else value + one
        return value

    def copies(p, m):
        level, target, _, count, slot = messages_of(plan[p])[m]
        run = pl.ds(slot, count)
        to = peer(chosen(plan[p][level], target))
        return [
            pltpu.make_async_remote_copy(
                src_ref=here, dst_ref=there, send_sem=a.at[p, m], recv_sem=b.at[p, m],
                device_id=to, device_id_type=MESH,
            )
            for here, there, a, b in (
                (sent.at[p, run], got.at[p, run], data_send, data_recv),
                (sent_top.at[p, m], got_top.at[p, m], top_send, top_recv),
            )
        ]

    def send(p, level):
        for m, (at, _, first, count, slot) in reversed(list(enumerate(messages_of(plan[p])))):
            if at != level:
                continue

            def pack(i):
                value = current(p, first + i, plan[p])
                if level:
                    value = value + arrived(p, level - 1, first + i)
                top = jnp.max(jnp.abs(value), axis=0, keepdims=True)
                scale = TOP / jnp.maximum(top, 2e-34)
                sent[p, slot + i] = jnp.round(value * scale).astype(jnp.int32).astype(jnp.int16)
                sent_top[p, m, pl.ds(i, 1), :] = top

            repeat(0, count, pack)
            for copy in copies(p, m):
                copy.start()

    def wait(p, level):
        for m, (at, *_) in enumerate(messages_of(plan[p])):
            if at == level:
                for copy in copies(p, m):
                    copy.wait_recv()

    def keep(p, level):
        count = [n for at, _, _, n, _ in messages_of(plan[p]) if at == level][0]
        if level + 1 < len(plan[p]):
            count >>= len(plan[p][level + 1])

        def add(i):
            value = arrived(p, level, i)
            for n, r in enumerate(rows_at(plan[p], i)):
                total[r, columns(p)] += value[n * own_rows : (n + 1) * own_rows]

        repeat(0, count, add)

    parts = len(plan)
    mine = pl.ds(pl.multiple_of((grp * members + mem) * own_rows, 8), own_rows)
    theirs = pl.ds(pl.multiple_of((partner[0] * members + mem) * own_rows, 8), own_rows)
    ends = []

    def advance(p, level):
        wait(p, level)
        if level + 1 < len(plan[p]):
            send(p, level + 1)
            keep(p, level)
            return
        keep(p, level)
        last[p] = total[theirs, columns(p)]
        at = pl.ds(pl.multiple_of(core * half + p * LANES, LANES), LANES)
        copy = pltpu.make_async_remote_copy(
            src_ref=last.at[p], dst_ref=out_ref.at[:, at],
            send_sem=end_send.at[p], recv_sem=end_recv.at[p],
            device_id=partner, device_id_type=MESH,
        )
        copy.start()
        ends.append(copy)
        out_ref[:, at] = total[mine, columns(p)]

    def multiply(low, high):
        def one(m, carry):
            tall = basis // 2
            at = pl.ds(pl.multiple_of(m * tall, LANES), tall)
            total[at, low:high] = jnp.dot(
                turned[at, :],
                both[:, pl.ds(pl.multiple_of(core * half + low, LANES), high - low)],
                preferred_element_type=jnp.float32,
            )
            return carry

        lax.fori_loop(0, 2, one, 0)

    step = [0] * parts
    made = 0
    for p in STEPS + list(range(parts)) * (2 + max(len(stages) for stages in plan)):
        if p >= parts or step[p] > len(plan[p]):
            continue
        if step[p] == 0:
            while chunks[made][0] <= p * LANES if made < len(chunks) else False:
                multiply(*chunks[made])
                made += 1
            send(p, 0)
        else:
            advance(p, step[p] - 1)
        step[p] += 1
    for copy in pair:
        copy.wait_send()
    for p in range(parts):
        for m in range(len(messages_of(plan[p]))):
            for copy in copies(p, m):
                copy.wait_send()
    for copy in ends:
        copy.wait()


NEAR, ROW = ("mem", 1), ("grp", 2)
ORDERS = ["xyab", "ayxb", "yabx", "yxab"]
STARTS = ["a2", "a3", "r1", "r0", "b1", "b2", "b3", "f0", "f1", "f2", "f3"]
ROUNDS = [0, 1, 2, 3] + [0, 2, 1, 3] * 3
CODE = 256.0
BEGIN = 8
SPARE = 16


def circle_plan(groups, members, parts):
    far = [("mem", 2 << k) for k in range(bits_of(members) - 1)]
    rows = [("grp", 2 << k) for k in range(bits_of(groups) - 1)]
    letters = {
        "x": [[NEAR]],
        "y": [[bit] for bit in rows],
        "a": [far[:1]],
        "b": [[bit] for bit in far[1:]],
        "z": [far[::-1]],
        "d": [rows + [NEAR]],
        "e": [[NEAR] + far[:1]],
        "f": [rows + far[:1]],
        "g": [rows + far[1:]],
        "h": [[NEAR] + far[1:]],
    }
    orders = [ORDERS[p % len(ORDERS)] for p in range(parts)]
    return [[stage for letter in order for stage in letters[letter]] for order in orders]


def place_of(groups, members, at):
    ladder, line = groups // 2, members // 2
    w, z = at // line, at % line
    z = line - 1 - z if w % 2 else z
    return (w, z, 0) if w < ladder else (2 * ladder - 1 - w, z, 1)


def moves_of(groups, members, own_rows, basis):
    unit = 2 * own_rows
    moves = []
    for low in range(0, basis, LANES):
        pieces, c = [], low
        while c < low + LANES:
            y, z, x = place_of(groups, members, c // unit)
            half, off = c % unit // own_rows, c % own_rows
            source = ((2 * y + half) * members + 2 * z + x) * own_rows + off
            count = min(own_rows - off, low + LANES - c, LANES - source % LANES)
            pieces.append((c - low, source // LANES, (c - low - source) % LANES))
            c += count
        moves.append(pieces)
    return moves


def circle_kernel(
    groups, members, plan, width, x_hbm, screen_ref, out_ref,
    x_ref, both, turned, raw, total, sent, got, sent_top, got_top, last, window, flipped, mirror, around,
    load, pair_send, pair_recv, data_send, data_recv, end_send, end_recv, flip_send, flip_recv,
):
    depth, basis = x_ref.shape
    own_rows = out_ref.shape[0]
    pieces = pair_send.shape[0]
    piece = depth // pieces
    loads = []
    for n in range(pieces):
        at = pl.ds(n * piece, piece)
        loads.append(pltpu.make_async_copy(x_hbm.at[at], x_ref.at[at], load.at[n]))
    loads[0].start()
    unit = 2 * own_rows
    chips = groups * members // 2
    line, ladder = members // 2, groups // 2
    reach = chips // 2
    tall = (own_rows + 15) // 16 * 16
    parts = len(plan)
    panels = basis // LANES
    occ_blocks = screen_ref.shape[1]
    grp, mem = lax.axis_index("grp"), lax.axis_index("mem")
    core = lax.rem(grp, 2)
    place = {"grp": grp - core, "mem": mem}
    lane = lax.broadcasted_iota(jnp.int32, (1, LANES), 1)
    swap = {NEAR: ROW, ROW: NEAR}

    def step_of(bit):
        axis, step = bit
        return step * (1 - 2 * lax.rem(place[axis] // step, 2))

    def moved(bits):
        there = dict(place)
        for bit in bits:
            other = swap.get(bit, bit)
            if other == bit:
                there[bit[0]] = there[bit[0]] + step_of(bit)
            else:
                there[bit[0]] = there[bit[0]] + step_of(bit) * (1 - core)
                there[other[0]] = there[other[0]] + step_of(other) * core
        return there["grp"], there["mem"]

    def peer(bits):
        g, m = moved(bits)
        return g + core, m

    def spot(g, m):
        y, z, x = g // 2, m // 2, lax.rem(m, 2)
        w = jnp.where(x == 1, 2 * ladder - 1 - y, y)
        return w * line + jnp.where(lax.rem(w, 2) == 1, line - 1 - z, z)

    def holder(at):
        w, z = at // line, lax.rem(at, line)
        z = jnp.where(lax.rem(w, 2) == 1, line - 1 - z, z)
        x = jnp.where(w >= ladder, 1, 0)
        y = jnp.where(w >= ladder, 2 * ladder - 1 - w, w)
        return 2 * y, 2 * z + x

    def chosen(bits, target):
        return tuple(b for t, b in enumerate(bits) if target >> (len(bits) - 1 - t) & 1)

    own = spot(grp, mem)
    partner = (grp + 1 - 2 * core, mem)
    barrier = pltpu.get_barrier_semaphore()
    met = {
        tuple(sorted(chosen(stages[level], target)))
        for stages in plan
        for level, target, *_ in messages_of(stages)
    }
    met |= {tuple(sorted(swap.get(b, b) for b in bits)) for bits in met}
    peers = [partner] + [peer(bits) for bits in sorted(met)]
    for other in peers:
        pl.semaphore_signal(barrier, inc=1, device_id=other, device_id_type=MESH)
    for copy in loads[1:]:
        copy.start()

    moves = moves_of(groups, members, own_rows, basis)

    def arrange(j, carry):
        for u in range(strips):
            row = j * strips + u
            at = pl.ds(pl.multiple_of(row * width, width), width)
            keep = screen_ref[0, lax.rem(row, occ_blocks)].astype(jnp.float32).astype(both.dtype)
            for n, pieces in enumerate(moves):
                value = None
                for first, m, shift in pieces:
                    piece = x_ref[at, columns(m)]
                    piece = pltpu.roll(piece, shift, 1) if shift else piece
                    value = piece if value is None else jnp.where(lane >= first, piece, value)
                value = value * keep
                both[at, columns(n)] = value
                if n < parts:
                    both[at, columns(panels + n)] = value
        return carry

    def columns(p):
        return slice(p * LANES, (p + 1) * LANES)

    strips = piece // width
    pair = []
    for n in range(pieces):
        with jax.named_scope(f"load{n}"):
            loads[n].wait()
        with jax.named_scope(f"arrange{n}"):
            count = piece // width // strips
            lax.fori_loop(n * count, (n + 1) * count, arrange, 0)
        if n == 0:
            with jax.named_scope("barrier"):
                pl.semaphore_wait(barrier, len(peers))
        pair.append(
            pltpu.make_async_remote_copy(
                src_ref=both.at[pl.ds(n * piece, piece), 0:basis],
                dst_ref=both.at[pl.ds(depth + n * piece, piece), 0:basis],
                send_sem=pair_send.at[n], recv_sem=pair_recv.at[n],
                device_id=partner, device_id_type=MESH,
            )
        )
        pair[-1].start()

    def turn(low, high):
        for k in range(low, high, LANES):
            turned[:, k : k + LANES] = both[k : k + LANES, 0:basis].T

    def rows_of(stages, index):
        order = [bit for bits in stages for bit in bits]
        there = dict(place)
        for t, bit in enumerate(order):
            flip = index // (1 << (len(order) - 1 - t)) % 2
            other = swap.get(bit, bit)
            if other == bit:
                there[bit[0]] = there[bit[0]] + flip * step_of(bit)
            else:
                there[bit[0]] = there[bit[0]] + flip * step_of(bit) * (1 - core)
                there[other[0]] = there[other[0]] + flip * step_of(other) * core
        return spot(there["grp"], there["mem"])

    def repeat(low, high, body):
        count = high - low
        by = 8 if count % 8 == 0 else count

        def step(t, carry):
            for u in range(by):
                body(low + t * by + u)
            return carry

        if count == by:
            step(0, 0)
        else:
            lax.fori_loop(0, count // by, step, 0)

    def panel_of(p):
        return jnp.where(core == 0, parts - 1 - p, parts + p)

    def block_at(s):
        return pl.ds(pl.multiple_of(s * unit, 16), unit)

    def start_of(s):
        start = s * unit + core * (parts * LANES)
        return jnp.where(start >= basis, start - basis, start)

    def multiply(s, low, high):
        at = pl.ds(pl.multiple_of(start_of(s) // LANES * LANES, LANES), (parts + 1) * LANES)
        value = jnp.dot(
            turned[block_at(s), low:high], both[low:high, at], preferred_element_type=jnp.float32
        )
        raw[block_at(s), :] = raw[block_at(s), :] + value if low else value

    def product(p, s):
        a = lax.rem(start_of(s), LANES)
        r = jnp.where(core == 0, parts - 1 - p, p)
        left = raw[block_at(s), pl.ds(pl.multiple_of(r * LANES, LANES), LANES)]
        right = raw[block_at(s), pl.ds(pl.multiple_of((r + 1) * LANES, LANES), LANES)]
        value = jnp.where(lane >= a, left, right)
        return pltpu.roll(value, jnp.where(a == 0, 0, LANES - a), 1)

    def current(p, index):
        return total[block_at(rows_of(plan[p], index)), columns(p)]

    def row_of(p, m):
        return messages_of(plan[p])[m][4] * unit + m * SPARE

    def block_of(p, m, index):
        return pl.ds(pl.multiple_of(row_of(p, m) + index * unit, 16), unit)

    def arrived(p, level, index):
        value = None
        for m, (at, *_) in enumerate(messages_of(plan[p])):
            if at == level:
                top = got_top[p, m, pl.ds(index, 1), :] * (1.0 / TOP)
                one = got[p, block_of(p, m, index), :].astype(jnp.int32).astype(jnp.float32) * top
                value = one if value is None else value + one
        return value

    def copy_to(p, m, here, there):
        level, target, *_ = messages_of(plan[p])[m]
        pltpu.make_async_remote_copy(
            src_ref=here, dst_ref=there, send_sem=data_send.at[p], recv_sem=data_recv.at[p, m],
            device_id=peer(chosen(plan[p][level], target)), device_id_type=MESH,
        ).start()

    def start_run(p, m, low, high):
        run = pl.ds(row_of(p, m) + low * unit, (high - low) * unit)
        copy_to(p, m, sent.at[p, run], got.at[p, run])

    def start_top(p, m):
        copy_to(p, m, sent_top.at[p, m], got_top.at[p, m])

    def crossing(p, index, bit=NEAR):
        order = [b for bits in plan[p] for b in bits]
        return index >> (len(order) - 1 - order.index(bit)) & 1

    def whole(p, m):
        count = messages_of(plan[p])[m][3]
        run = pl.ds(row_of(p, m), count * unit + SPARE)
        return pltpu.make_async_remote_copy(
            src_ref=sent.at[p, run], dst_ref=got.at[p, run],
            send_sem=data_send.at[p], recv_sem=data_recv.at[p, m],
            device_id=partner, device_id_type=MESH,
        )

    def all_sent(p):
        rows = row_of(p, 0) + (chips - 1) * unit + len(messages_of(plan[p])) * SPARE
        pltpu.make_async_remote_copy(
            src_ref=sent.at[p, pl.ds(0, rows)], dst_ref=got.at[p, pl.ds(0, rows)],
            send_sem=data_send.at[p], recv_sem=data_recv.at[p, 0],
            device_id=partner, device_id_type=MESH,
        ).wait_send()

    def multiply_all(first, last, low, high):
        def one(t, carry):
            for u in range(4):
                multiply(rows_of(plan[0], first + t * 4 + u), low, high)
            return carry

        lax.fori_loop(0, (last - first) // 4, one, 0)

    def pack(p, m, i):
        level, _, first, _, _ = messages_of(plan[p])[m]
        if level:
            value = current(p, first + i) + arrived(p, level - 1, first + i)
        else:
            value = product(p, rows_of(plan[p], first + i))
        top = jnp.max(jnp.abs(value), axis=0, keepdims=True)
        scale = TOP / jnp.maximum(top, 2e-34)
        packed = jnp.round(value * scale).astype(jnp.int32).astype(jnp.int16)
        sent[p, block_of(p, m, i), :] = packed
        sent_top[p, m, pl.ds(i, 1), :] = top

    def send(p, level):
        for m, (at, _, _, count, _) in reversed(list(enumerate(messages_of(plan[p])))):
            if at == level:
                repeat(0, count, functools.partial(pack, p, m))
                start_run(p, m, 0, count)
                start_top(p, m)

    def send_first(p, group, low=0, high=None):
        for m, (at, _, first, count, _) in enumerate(messages_of(plan[p])):
            if at:
                continue
            chunk = [i for i in range(count) if crossing(p, first + i) == 1 - group]
            ends_here = group == 1 or len(chunk) == count
            chunk = chunk[low:high]
            for i in chunk:
                pack(p, m, i)
            runs = []
            for i in chunk:
                if runs and runs[-1][1] == i:
                    runs[-1][1] = i + 1
                else:
                    runs.append([i, i + 1])
            for run in runs:
                start_run(p, m, *run)
            if chunk and ends_here and (high is None or high >= count):
                start_top(p, m)

    def remaining(p, level):
        count = [n for at, _, _, n, _ in messages_of(plan[p]) if at == level][0]
        return count

    def fill(p):
        def one(i):
            s = rows_of(plan[p], i)
            total[block_at(s), columns(p)] = product(p, s)

        repeat(0, remaining(p, 0), one)

    def wait(p, level):
        for m, (at, *_) in enumerate(messages_of(plan[p])):
            if at == level:
                whole(p, m).wait_recv()

    def keep(p, level):
        count = remaining(p, level)
        if level + 1 < len(plan[p]):
            count >>= len(plan[p][level + 1])

        def add(i):
            total[block_at(rows_of(plan[p], i)), columns(p)] += arrived(p, level, i)

        repeat(0, count, add)

    def cuts(p, side):
        q = parts - 1 - p if side == 0 else parts + p
        result = []
        for k in range(1, reach):
            for half in range(2):
                base = k * unit + (unit - tall) * half
                low, high = max(base, q * LANES), min(base + tall, (q + 1) * LANES)
                if low < high:
                    result.append((k, half, low - q * LANES, low - base, high - low))
        return result

    def flips(p, side):
        for k, half, here, there, count in cuts(p, side):
            g, m = holder(lax.rem(own + k, chips))
            yield pltpu.make_async_remote_copy(
                src_ref=flipped.at[pl.ds(p * LANES + here, count)],
                dst_ref=mirror.at[pl.ds((k - 1) * tall + there, count)],
                send_sem=flip_send, recv_sem=flip_recv,
                device_id=(g + half, m), device_id_type=MESH,
            )

    def flips_like(ref, count):
        run = pl.ds(0, count)
        return pltpu.make_async_remote_copy(
            src_ref=ref.at[run], dst_ref=ref.at[run], send_sem=flip_send, recv_sem=flip_recv,
            device_id=partner, device_id_type=MESH,
        )

    def ends(p):
        q = panel_of(p)
        at = pl.ds(pl.multiple_of(q * LANES, LANES), LANES)
        return pltpu.make_async_remote_copy(
            src_ref=last.at[p], dst_ref=window.at[:, at],
            send_sem=end_send, recv_sem=end_recv,
            device_id=partner, device_id_type=MESH,
        )

    def all_ends():
        at = pl.ds(pl.multiple_of((1 - core) * parts * LANES, LANES), parts * LANES)
        return pltpu.make_async_remote_copy(
            src_ref=window.at[:, at], dst_ref=window.at[:, at],
            send_sem=end_send, recv_sem=end_recv,
            device_id=partner, device_id_type=MESH,
        )

    def finish(p):
        mine = pl.ds(pl.multiple_of(own * unit + core * own_rows, 8), own_rows)
        theirs = pl.ds(pl.multiple_of(own * unit + (1 - core) * own_rows, 8), own_rows)
        last[p] = total[theirs, columns(p)]
        ends(p).start()
        if cuts(p, 0) or cuts(p, 1):
            value = total[block_at(own), columns(p)]
            top = jnp.max(jnp.abs(value), axis=0, keepdims=True)
            code = jnp.ceil(jnp.log2(jnp.maximum(top, 2e-34)) * CODE) + 1.0
            scale = TOP * jnp.exp2(code * (-1.0 / CODE))
            code = jnp.broadcast_to(code, (LANES - unit, LANES))
            value = jnp.concatenate([jnp.round(value * scale), code], axis=0).T
            flipped[p * LANES : (p + 1) * LANES, :] = value.astype(jnp.int32).astype(jnp.int16)
        for side in range(2):
            if cuts(p, side):
                @pl.when(core == side)
                def _():
                    for copy in flips(p, side):
                        copy.start()
        at = pl.ds(pl.multiple_of(panel_of(p) * LANES, LANES), LANES)
        window[:, at] = total[mine, columns(p)]

    early = depth // LANES * LANES
    with jax.named_scope("turn"):
        turn(0, early)
    later = chips - BEGIN
    with jax.named_scope("begin"):
        multiply_all(later, chips, 0, early)
    done = 0
    for low in range(early, 2 * depth, LANES):
        while done < pieces and low + LANES > depth + done * piece:
            with jax.named_scope(f"pair{done}"):
                pair[done].wait_recv()
            done += 1
        with jax.named_scope(f"turn{low}"):
            if low + LANES > depth:
                rows = slice(max(low, depth), low + LANES)
                both[rows, basis:] = both[rows, : parts * LANES]
            turn(low, low + LANES)
    half = (chips + later) // 2
    with jax.named_scope("multiply"):
        multiply_all(later, half, early, 2 * depth)
    with jax.named_scope("send0_0"):
        send_first(0, 0, 0, half - later)
    with jax.named_scope("multiply2"):
        multiply_all(half, chips, early, 2 * depth)
    with jax.named_scope("send1_0a"):
        send_first(1, 0)
    with jax.named_scope("send0_0b"):
        send_first(0, 0, half - later, chips)
    level = [0] * parts
    filled = [False] * parts
    for word in STARTS + [str(p) for p in ROUNDS + list(range(parts)) * 8]:
        if word[0] == "r":
            with jax.named_scope("rest" + word[1]):
                for i in range(later):
                    if crossing(0, i, ("mem", 2)) == int(word[1]):
                        multiply(rows_of(plan[0], i), 0, 2 * depth)
            continue
        p = int(word[-1])
        if p >= parts or level[p] >= len(plan[p]):
            continue
        if word[0] in "ab":
            with jax.named_scope(f"send{word}"):
                send_first(p, "ab".index(word[0]))
            continue
        if not filled[p]:
            with jax.named_scope(f"fill{p}"):
                fill(p)
            filled[p] = True
        if word[0] == "f":
            continue
        with jax.named_scope(f"wait{p}_{level[p]}"):
            wait(p, level[p])
        if level[p] + 1 < len(plan[p]):
            with jax.named_scope(f"send{p}_{level[p] + 1}"):
                send(p, level[p] + 1)
        with jax.named_scope(f"keep{p}_{level[p]}"):
            keep(p, level[p])
        level[p] += 1
        if level[p] == len(plan[p]):
            with jax.named_scope(f"finish{p}"):
                finish(p)

    with jax.named_scope("ends"):
        all_ends().wait_recv()
    for k in range(reach + 1):
        n, a = k * unit // LANES, k * unit % LANES
        value = window[:, columns(n)]
        if a:
            if a + unit > LANES:
                value = jnp.where(lane >= a, value, window[:, columns(n + 1)])
            value = pltpu.roll(value, LANES - a, 1)
        around[k] = value
    with jax.named_scope("flips"):
        flips_like(mirror, (reach - 1) * tall).wait_recv()
    for k in range(1, reach):
        low = (k - 1) * tall
        value = mirror[low : low + tall, :].astype(jnp.int32).astype(jnp.float32)
        value = jnp.where(core == 0, value[:own_rows], value[tall - own_rows :])
        scale = jnp.exp2(value[:, unit : unit + 1] * (1.0 / CODE)) * (1.0 / TOP)
        around[chips - k] = value * scale
    with jax.named_scope("out"):
      for n in range(panels):
        value, c = None, n * LANES
        while c < (n + 1) * LANES:
            b, off = c // own_rows, c % own_rows
            g, m = b // members, b % members
            s = next(s for s in range(chips) if place_of(groups, members, s) == (g // 2, m // 2, m % 2))
            piece = around[lax.rem(s - own + chips, chips)]
            shift = (c - n * LANES - (g % 2 * own_rows + off)) % LANES
            piece = pltpu.roll(piece, shift, 1) if shift else piece
            value = piece if value is None else jnp.where(lane >= c - n * LANES, piece, value)
            c += min(own_rows - off, (n + 1) * LANES - c)
        out_ref[:, columns(n)] = value
    with jax.named_scope("sents"):
        for copy in pair:
            copy.wait_send()
        for p in range(parts):
            all_sent(p)
        for side in range(2):
            count = sum(cut[4] for p in range(parts) for cut in cuts(p, side))
            pl.when(core == side)(flips_like(flipped, count).wait_send)
        all_ends().wait_send()


def circle_call(groups, members, rows, screen, own_rows, width):
    depth, basis = rows.shape
    unit = 2 * own_rows
    chips = groups * members // 2
    parts = -(-(chips // 2 + 1) * unit // LANES) // 2
    plan = circle_plan(groups, members, parts)
    levels = max(len(messages_of(stages)) for stages in plan)
    places = SPARE // 2
    deep = (chips - 1) * unit + levels * SPARE
    tall = (own_rows + 15) // 16 * 16
    pieces = 4
    dma = pltpu.SemaphoreType.DMA
    vmem = pl.BlockSpec(memory_space=pltpu.VMEM)
    return pl.pallas_call(
        functools.partial(circle_kernel, groups, members, plan, width),
        out_shape=pltpu.VMEM((own_rows, basis), jnp.float32),
        in_specs=[pl.BlockSpec(memory_space=pl.ANY), pl.BlockSpec(memory_space=pltpu.SMEM)],
        out_specs=vmem,
        scratch_shapes=[
            pltpu.VMEM((depth, basis), jnp.bfloat16),
            pltpu.VMEM((2 * depth, basis + parts * LANES), jnp.bfloat16),
            pltpu.VMEM((basis, 2 * depth), jnp.bfloat16),
            pltpu.VMEM((basis, (parts + 1) * LANES), jnp.float32),
            pltpu.VMEM((basis, parts * LANES), jnp.float32),
            pltpu.VMEM((parts, deep, LANES), jnp.int16),
            pltpu.VMEM((parts, deep, LANES), jnp.int16),
            pltpu.VMEM((parts, levels, places, LANES), jnp.float32),
            pltpu.VMEM((parts, levels, places, LANES), jnp.float32),
            pltpu.VMEM((parts, own_rows, LANES), jnp.float32),
            pltpu.VMEM((own_rows, 2 * parts * LANES), jnp.float32),
            pltpu.VMEM((parts * LANES, LANES), jnp.int16),
            pltpu.VMEM(((chips // 2 - 1) * tall, LANES), jnp.int16),
            pltpu.VMEM((chips, own_rows, LANES), jnp.float32),
            dma((pieces,)), dma((pieces,)), dma((pieces,)),
            dma((parts,)), dma((parts, levels)), dma, dma, dma, dma,
        ],
        compiler_params=pltpu.CompilerParams(
            collective_id=1, has_side_effects=True, vmem_limit_bytes=60 * 1024 * 1024
        ),
    )(rows, screen)


def circle_fits(groups, members, own_rows, basis, depth, width):
    unit = 2 * own_rows
    chips = groups * members // 2
    panels = -(-(chips // 2 + 1) * unit // LANES)
    return (
        groups >= 4 and members >= 4 and 64 < unit < LANES and unit % 16 == 0
        and chips // 2 <= SPARE // 2
        and basis % 256 == 0 and panels % 2 == 0 and depth % (4 * width) == 0
    )


def solution(mesh):
    groups, members = mesh.shape["grp"], mesh.shape["mem"]

    def on_device(factors, screen):
        aux_rows, occ_count, basis = factors.shape
        depth = aux_rows * occ_count
        devices = groups * members
        real_rows = basis // devices
        own_rows = (real_rows + 7) // 8 * 8
        rows = factors.reshape(depth, basis)
        if own_rows != real_rows:
            rows = rows.reshape(depth, devices, real_rows)
            rows = jnp.pad(rows, ((0, 0), (0, 0), (0, own_rows - real_rows)))
            basis = devices * own_rows
            rows = rows.reshape(depth, basis)
        width = occ_count // screen.shape[1]
        if own_rows == real_rows and circle_fits(groups, members, own_rows, basis, depth, width):
            return circle_call(groups, members, rows, screen, own_rows, width)
        half = basis // 2
        parts = half // LANES
        plan = plan_for(groups, members, parts)
        chunks = [(low, min(low + 2 * LANES, half)) for low in range(0, half, 2 * LANES)]
        chips = groups * members // 2
        levels = max(len(messages_of(stages)) for stages in plan)
        block = 2 * own_rows
        places = max(8, chips // 2)
        dma = pltpu.SemaphoreType.DMA
        vmem = pl.BlockSpec(memory_space=pltpu.VMEM)
        result = pl.pallas_call(
            functools.partial(kernel, groups, members, plan, chunks, occ_count // screen.shape[1]),
            out_shape=pltpu.VMEM((own_rows, basis), jnp.float32),
            in_specs=[vmem, pl.BlockSpec(memory_space=pltpu.SMEM)],
            out_specs=vmem,
            scratch_shapes=[
                pltpu.VMEM((2 * depth, basis), jnp.bfloat16),
                pltpu.VMEM((basis, 2 * depth), jnp.bfloat16),
                pltpu.VMEM((basis, half), jnp.float32),
                pltpu.VMEM((parts, chips - 1, block, LANES), jnp.int16),
                pltpu.VMEM((parts, chips - 1, block, LANES), jnp.int16),
                pltpu.VMEM((parts, levels, places, LANES), jnp.float32),
                pltpu.VMEM((parts, levels, places, LANES), jnp.float32),
                pltpu.VMEM((parts, own_rows, LANES), jnp.float32),
                dma((2,)), dma((2,)),
                dma((parts, levels)), dma((parts, levels)),
                dma((parts, levels)), dma((parts, levels)),
                dma((parts,)), dma((parts,)),
            ],
            compiler_params=pltpu.CompilerParams(
                collective_id=0, has_side_effects=True, vmem_limit_bytes=60 * 1024 * 1024
            ),
        )(rows, screen)
        if own_rows != real_rows:
            result = result[:real_rows].reshape(real_rows, devices, own_rows)[:, :, :real_rows]
            result = result.reshape(real_rows, devices * real_rows)
        return result

    placed = (P(("grp", "mem"), None, None), P(("grp", "mem"), None))
    return jax.shard_map(
        on_device, mesh=mesh, in_specs=placed, out_specs=P(("grp", "mem"), None), check_vma=False
    )
```

```python
import functools

import jax
import jax.numpy as jnp
from jax import lax
from jax.experimental import pallas as pl
from jax.experimental.pallas import tpu as pltpu
from jax.sharding import PartitionSpec as P

LANES = 128
TOP = 32767.0
KINDS = "DGCFGFG"
STEPS = [0, 1, 2, 3, 4, 0, 1, 5, 6, 2, 3, 4, 0, 1, 5, 6]
MESH = pl.DeviceIdType.MESH


def bits_of(size):
    return size.bit_length() - 1


def plan_for(groups, members, parts):
    near = [[("mem", 1)]]
    rows = [[("grp", 2 << k)] for k in range(bits_of(groups) - 1)]
    far = [("mem", 2 << k) for k in range(bits_of(members) - 1)]
    single = [[bit] for bit in far]
    direct = [far[k : k + 2][::-1] for k in range(0, len(far), 2)]
    kinds = {
        "A": near + rows + direct,
        "B": rows + near + direct,
        "C": single + near + rows,
        "D": near + single + rows,
        "E": rows + single + near,
        "F": near + rows + single,
        "G": rows + near + single,
    }
    return [kinds[KINDS[p % len(KINDS)]] for p in range(parts)]


def messages_of(stages):
    left = 1
    for bits in stages:
        left <<= len(bits)
    result, slot = [], 0
    for level, bits in enumerate(stages):
        left >>= len(bits)
        for target in range(1, 1 << len(bits)):
            result.append((level, target, target * left, left, slot))
            slot += left
    return result


def kernel(
    groups, members, plan, chunks, width, x_ref, screen_ref, out_ref,
    both, turned, total, sent, got, sent_top, got_top, last,
    pair_send, pair_recv, data_send, data_recv, top_send, top_recv, end_send, end_recv,
):
    depth, basis = x_ref.shape
    own_rows = out_ref.shape[0]
    half = basis // 2
    occ_blocks = screen_ref.shape[1]
    grp, mem = lax.axis_index("grp"), lax.axis_index("mem")
    core = lax.rem(grp, 2)
    place = {"grp": grp, "mem": mem}
    def peer(bits):
        there = dict(place)
        for axis, step in bits:
            bit = lax.rem(place[axis] // step, 2)
            there[axis] = there[axis] + (1 - 2 * bit) * step
        return there["grp"], there["mem"]

    def chosen(bits, target):
        return tuple(b for t, b in enumerate(bits) if target >> (len(bits) - 1 - t) & 1)

    partner = peer([("grp", 1)])
    barrier = pltpu.get_barrier_semaphore()
    met = {
        tuple(sorted(chosen(stages[level], target)))
        for stages in plan
        for level, target, *_ in messages_of(stages)
    }
    peers = [partner] + [peer(bits) for bits in sorted(met)]
    for other in peers:
        pl.semaphore_signal(barrier, inc=1, device_id=other, device_id_type=MESH)


    def mask(j, carry):
        at = pl.ds(pl.multiple_of(j * width, width), width)
        keep = screen_ref[0, lax.rem(j, occ_blocks)].astype(jnp.float32)
        both[at, :] = (x_ref[at, :].astype(jnp.float32) * keep).astype(both.dtype)
        return carry

    pieces = 2
    piece = depth // pieces
    pair = []
    for n in range(pieces):
        lax.fori_loop(n * piece // width, (n + 1) * piece // width, mask, 0)
        if n == 0:
            pl.semaphore_wait(barrier, len(peers))
        pair.append(
            pltpu.make_async_remote_copy(
                src_ref=both.at[pl.ds(n * piece, piece)],
                dst_ref=both.at[pl.ds(depth + n * piece, piece)],
                send_sem=pair_send.at[n], recv_sem=pair_recv.at[n],
                device_id=partner, device_id_type=MESH,
            )
        )
        pair[-1].start()

    def turn(low, high):
        def one(m, carry):
            at = pl.ds(pl.multiple_of(m * 256, 256), 256)
            for k in range(low, high, LANES):
                turned[at, k : k + LANES] = both[k : k + LANES, at].T
            return carry

        lax.fori_loop(0, basis // 256, one, 0)

    early = depth // LANES * LANES
    turn(0, early)
    for copy in pair:
        copy.wait_recv()
    turn(early, 2 * depth)

    def rows_at(stages, index):
        order = [bit for bits in stages for bit in bits]
        at = {"grp": grp - core, "mem": mem}
        for t, (axis, step) in enumerate(order):
            flip = index // (1 << (len(order) - 1 - t)) % 2
            bit = lax.rem(place[axis] // step, 2)
            at[axis] = at[axis] + flip * (1 - 2 * bit) * step
        first = (at["grp"] * members + at["mem"]) * own_rows
        second = first + members * own_rows
        return [pl.ds(pl.multiple_of(r, 8), own_rows) for r in (first, second)]

    def repeat(low, high, body):
        count = high - low
        by = 4 if count % 4 == 0 else count

        def step(t, carry):
            for u in range(by):
                body(low + t * by + u)
            return carry

        if count == by:
            step(0, 0)
        else:
            lax.fori_loop(0, count // by, step, 0)

    def columns(p):
        return slice(p * LANES, (p + 1) * LANES)

    def current(p, index, order):
        return jnp.concatenate([total[r, columns(p)] for r in rows_at(order, index)], axis=0)

    def arrived(p, level, index):
        value = None
        for m, (at, _, _, _, slot) in enumerate(messages_of(plan[p])):
            if at == level:
                top = got_top[p, m, pl.ds(index, 1), :] * (1.0 / TOP)
                one = got[p, slot + index].astype(jnp.int32).astype(jnp.float32) * top
                value = one if value is None else value + one
        return value

    def copies(p, m):
        level, target, _, count, slot = messages_of(plan[p])[m]
        run = pl.ds(slot, count)
        to = peer(chosen(plan[p][level], target))
        return [
            pltpu.make_async_remote_copy(
                src_ref=here, dst_ref=there, send_sem=a.at[p, m], recv_sem=b.at[p, m],
                device_id=to, device_id_type=MESH,
            )
            for here, there, a, b in (
                (sent.at[p, run], got.at[p, run], data_send, data_recv),
                (sent_top.at[p, m], got_top.at[p, m], top_send, top_recv),
            )
        ]

    def send(p, level):
        for m, (at, _, first, count, slot) in reversed(list(enumerate(messages_of(plan[p])))):
            if at != level:
                continue

            def pack(i):
                value = current(p, first + i, plan[p])
                if level:
                    value = value + arrived(p, level - 1, first + i)
                top = jnp.max(jnp.abs(value), axis=0, keepdims=True)
                scale = TOP / jnp.maximum(top, 2e-34)
                sent[p, slot + i] = jnp.round(value * scale).astype(jnp.int32).astype(jnp.int16)
                sent_top[p, m, pl.ds(i, 1), :] = top

            repeat(0, count, pack)
            for copy in copies(p, m):
                copy.start()

    def wait(p, level):
        for m, (at, *_) in enumerate(messages_of(plan[p])):
            if at == level:
                for copy in copies(p, m):
                    copy.wait_recv()

    def keep(p, level):
        count = [n for at, _, _, n, _ in messages_of(plan[p]) if at == level][0]
        if level + 1 < len(plan[p]):
            count >>= len(plan[p][level + 1])

        def add(i):
            value = arrived(p, level, i)
            for n, r in enumerate(rows_at(plan[p], i)):
                total[r, columns(p)] += value[n * own_rows : (n + 1) * own_rows]

        repeat(0, count, add)

    parts = len(plan)
    mine = pl.ds(pl.multiple_of((grp * members + mem) * own_rows, 8), own_rows)
    theirs = pl.ds(pl.multiple_of((partner[0] * members + mem) * own_rows, 8), own_rows)
    ends = []

    def advance(p, level):
        wait(p, level)
        if level + 1 < len(plan[p]):
            send(p, level + 1)
            keep(p, level)
            return
        keep(p, level)
        last[p] = total[theirs, columns(p)]
        at = pl.ds(pl.multiple_of(core * half + p * LANES, LANES), LANES)
        copy = pltpu.make_async_remote_copy(
            src_ref=last.at[p], dst_ref=out_ref.at[:, at],
            send_sem=end_send.at[p], recv_sem=end_recv.at[p],
            device_id=partner, device_id_type=MESH,
        )
        copy.start()
        ends.append(copy)
        out_ref[:, at] = total[mine, columns(p)]

    def multiply(low, high):
        def one(m, carry):
            tall = basis // 2
            at = pl.ds(pl.multiple_of(m * tall, LANES), tall)
            total[at, low:high] = jnp.dot(
                turned[at, :],
                both[:, pl.ds(pl.multiple_of(core * half + low, LANES), high - low)],
                preferred_element_type=jnp.float32,
            )
            return carry

        lax.fori_loop(0, 2, one, 0)

    step = [0] * parts
    made = 0
    for p in STEPS + list(range(parts)) * (2 + max(len(stages) for stages in plan)):
        if p >= parts or step[p] > len(plan[p]):
            continue
        if step[p] == 0:
            while chunks[made][0] <= p * LANES if made < len(chunks) else False:
                multiply(*chunks[made])
                made += 1
            send(p, 0)
        else:
            advance(p, step[p] - 1)
        step[p] += 1
    for copy in pair:
        copy.wait_send()
    for p in range(parts):
        for m in range(len(messages_of(plan[p]))):
            for copy in copies(p, m):
                copy.wait_send()
    for copy in ends:
        copy.wait()


NEAR, ROW = ("mem", 1), ("grp", 2)
ORDERS = ["xyab", "ayxb", "yabx", "yxab"]
STARTS = ["a2", "a3", "r1", "r0", "b1", "b2", "b3", "f0", "f1", "f2", "f3"]
ROUNDS = [0, 1, 2, 3] + [0, 2, 1, 3] * 3
CODE = 256.0
BEGIN = 8
SPARE = 16
PIECES = 6


def circle_plan(groups, members, parts):
    far = [("mem", 2 << k) for k in range(bits_of(members) - 1)]
    rows = [("grp", 2 << k) for k in range(bits_of(groups) - 1)]
    letters = {
        "x": [[NEAR]],
        "y": [[bit] for bit in rows],
        "a": [far[:1]],
        "b": [[bit] for bit in far[1:]],
        "z": [far[::-1]],
        "d": [rows + [NEAR]],
        "e": [[NEAR] + far[:1]],
        "f": [rows + far[:1]],
        "g": [rows + far[1:]],
        "h": [[NEAR] + far[1:]],
    }
    orders = [ORDERS[p % len(ORDERS)] for p in range(parts)]
    return [[stage for letter in order for stage in letters[letter]] for order in orders]


def place_of(groups, members, at):
    ladder, line = groups // 2, members // 2
    w, z = at // line, at % line
    z = line - 1 - z if w % 2 else z
    return (w, z, 0) if w < ladder else (2 * ladder - 1 - w, z, 1)


def moves_of(groups, members, own_rows, basis):
    unit = 2 * own_rows
    moves = []
    for low in range(0, basis, LANES):
        pieces, c = [], low
        while c < low + LANES:
            y, z, x = place_of(groups, members, c // unit)
            half, off = c % unit // own_rows, c % own_rows
            source = ((2 * y + half) * members + 2 * z + x) * own_rows + off
            count = min(own_rows - off, low + LANES - c, LANES - source % LANES)
            pieces.append((c - low, source // LANES, (c - low - source) % LANES))
            c += count
        moves.append(pieces)
    return moves


def circle_kernel(
    groups, members, plan, width, x_hbm, screen_ref, out_ref,
    x_ref, both, turned, raw, total, sent, got, sent_top, got_top, last, window, flipped, mirror, around,
    load, pair_send, pair_recv, data_send, data_recv, end_send, end_recv, flip_send, flip_recv,
):
    depth, basis = x_ref.shape
    own_rows = out_ref.shape[0]
    pieces = pair_send.shape[0]
    piece = depth // pieces
    loads = []
    for n in range(pieces):
        at = pl.ds(n * piece, piece)
        loads.append(pltpu.make_async_copy(x_hbm.at[at], x_ref.at[at], load.at[n]))
    loads[0].start()
    unit = 2 * own_rows
    chips = groups * members // 2
    line, ladder = members // 2, groups // 2
    reach = chips // 2
    tall = (own_rows + 15) // 16 * 16
    parts = len(plan)
    panels = basis // LANES
    occ_blocks = screen_ref.shape[1]
    grp, mem = lax.axis_index("grp"), lax.axis_index("mem")
    core = lax.rem(grp, 2)
    place = {"grp": grp - core, "mem": mem}
    lane = lax.broadcasted_iota(jnp.int32, (1, LANES), 1)
    swap = {NEAR: ROW, ROW: NEAR}

    def step_of(bit):
        axis, step = bit
        return step * (1 - 2 * lax.rem(place[axis] // step, 2))

    def moved(bits):
        there = dict(place)
        for bit in bits:
            other = swap.get(bit, bit)
            if other == bit:
                there[bit[0]] = there[bit[0]] + step_of(bit)
            else:
                there[bit[0]] = there[bit[0]] + step_of(bit) * (1 - core)
                there[other[0]] = there[other[0]] + step_of(other) * core
        return there["grp"], there["mem"]

    def peer(bits):
        g, m = moved(bits)
        return g + core, m

    def spot(g, m):
        y, z, x = g // 2, m // 2, lax.rem(m, 2)
        w = jnp.where(x == 1, 2 * ladder - 1 - y, y)
        return w * line + jnp.where(lax.rem(w, 2) == 1, line - 1 - z, z)

    def holder(at):
        w, z = at // line, lax.rem(at, line)
        z = jnp.where(lax.rem(w, 2) == 1, line - 1 - z, z)
        x = jnp.where(w >= ladder, 1, 0)
        y = jnp.where(w >= ladder, 2 * ladder - 1 - w, w)
        return 2 * y, 2 * z + x

    def chosen(bits, target):
        return tuple(b for t, b in enumerate(bits) if target >> (len(bits) - 1 - t) & 1)

    own = spot(grp, mem)
    partner = (grp + 1 - 2 * core, mem)
    barrier = pltpu.get_barrier_semaphore()
    met = {
        tuple(sorted(chosen(stages[level], target)))
        for stages in plan
        for level, target, *_ in messages_of(stages)
    }
    met |= {tuple(sorted(swap.get(b, b) for b in bits)) for bits in met}
    peers = [partner] + [peer(bits) for bits in sorted(met)]
    for other in peers:
        pl.semaphore_signal(barrier, inc=1, device_id=other, device_id_type=MESH)
    for copy in loads[1:]:
        copy.start()

    moves = moves_of(groups, members, own_rows, basis)

    def arrange(j, carry):
        for u in range(strips):
            row = j * strips + u
            at = pl.ds(pl.multiple_of(row * width, width), width)
            keep = screen_ref[0, lax.rem(row, occ_blocks)].astype(jnp.float32).astype(both.dtype)
            for n, pieces in enumerate(moves):
                value = None
                for first, m, shift in pieces:
                    piece = x_ref[at, columns(m)]
                    piece = pltpu.roll(piece, shift, 1) if shift else piece
                    value = piece if value is None else jnp.where(lane >= first, piece, value)
                value = value * keep
                both[at, columns(n)] = value
                if n < parts:
                    both[at, columns(panels + n)] = value
        return carry

    def columns(p):
        return slice(p * LANES, (p + 1) * LANES)

    strips = piece // width
    pair = []
    for n in range(pieces):
        with jax.named_scope(f"load{n}"):
            loads[n].wait()
        with jax.named_scope(f"arrange{n}"):
            count = piece // width // strips
            lax.fori_loop(n * count, (n + 1) * count, arrange, 0)
        if n == 0:
            with jax.named_scope("barrier"):
                pl.semaphore_wait(barrier, len(peers))
        pair.append(
            pltpu.make_async_remote_copy(
                src_ref=both.at[pl.ds(n * piece, piece), 0:basis],
                dst_ref=both.at[pl.ds(depth + n * piece, piece), 0:basis],
                send_sem=pair_send.at[n], recv_sem=pair_recv.at[n],
                device_id=partner, device_id_type=MESH,
            )
        )
        pair[-1].start()

    def turn(low, high):
        for k in range(low, high, LANES):
            turned[:, k : k + LANES] = both[k : k + LANES, 0:basis].T

    def rows_of(stages, index):
        order = [bit for bits in stages for bit in bits]
        there = dict(place)
        for t, bit in enumerate(order):
            flip = index // (1 << (len(order) - 1 - t)) % 2
            other = swap.get(bit, bit)
            if other == bit:
                there[bit[0]] = there[bit[0]] + flip * step_of(bit)
            else:
                there[bit[0]] = there[bit[0]] + flip * step_of(bit) * (1 - core)
                there[other[0]] = there[other[0]] + flip * step_of(other) * core
        return spot(there["grp"], there["mem"])

    def repeat(low, high, body):
        count = high - low
        by = 8 if count % 8 == 0 else count

        def step(t, carry):
            for u in range(by):
                body(low + t * by + u)
            return carry

        if count == by:
            step(0, 0)
        else:
            lax.fori_loop(0, count // by, step, 0)

    def panel_of(p):
        return jnp.where(core == 0, parts - 1 - p, parts + p)

    def block_at(s):
        return pl.ds(pl.multiple_of(s * unit, 16), unit)

    def start_of(s):
        start = s * unit + core * (parts * LANES)
        return jnp.where(start >= basis, start - basis, start)

    def multiply(s, low, high):
        at = pl.ds(pl.multiple_of(start_of(s) // LANES * LANES, LANES), (parts + 1) * LANES)
        value = jnp.dot(
            turned[block_at(s), low:high], both[low:high, at], preferred_element_type=jnp.float32
        )
        raw[block_at(s), :] = raw[block_at(s), :] + value if low else value

    def product(p, s):
        a = lax.rem(start_of(s), LANES)
        r = jnp.where(core == 0, parts - 1 - p, p)
        left = raw[block_at(s), pl.ds(pl.multiple_of(r * LANES, LANES), LANES)]
        right = raw[block_at(s), pl.ds(pl.multiple_of((r + 1) * LANES, LANES), LANES)]
        value = jnp.where(lane >= a, left, right)
        return pltpu.roll(value, jnp.where(a == 0, 0, LANES - a), 1)

    def current(p, index):
        return total[block_at(rows_of(plan[p], index)), columns(p)]

    def row_of(p, m):
        return messages_of(plan[p])[m][4] * unit + m * SPARE

    def block_of(p, m, index):
        return pl.ds(pl.multiple_of(row_of(p, m) + index * unit, 16), unit)

    def arrived(p, level, index):
        value = None
        for m, (at, *_) in enumerate(messages_of(plan[p])):
            if at == level:
                top = got_top[p, m, pl.ds(index, 1), :] * (1.0 / TOP)
                one = got[p, block_of(p, m, index), :].astype(jnp.int32).astype(jnp.float32) * top
                value = one if value is None else value + one
        return value

    def copy_to(p, m, here, there):
        level, target, *_ = messages_of(plan[p])[m]
        pltpu.make_async_remote_copy(
            src_ref=here, dst_ref=there, send_sem=data_send.at[p], recv_sem=data_recv.at[p, m],
            device_id=peer(chosen(plan[p][level], target)), device_id_type=MESH,
        ).start()

    def start_run(p, m, low, high):
        run = pl.ds(row_of(p, m) + low * unit, (high - low) * unit)
        copy_to(p, m, sent.at[p, run], got.at[p, run])

    def start_top(p, m):
        copy_to(p, m, sent_top.at[p, m], got_top.at[p, m])

    def crossing(p, index, bit=NEAR):
        order = [b for bits in plan[p] for b in bits]
        return index >> (len(order) - 1 - order.index(bit)) & 1

    def whole(p, m):
        count = messages_of(plan[p])[m][3]
        run = pl.ds(row_of(p, m), count * unit + SPARE)
        return pltpu.make_async_remote_copy(
            src_ref=sent.at[p, run], dst_ref=got.at[p, run],
            send_sem=data_send.at[p], recv_sem=data_recv.at[p, m],
            device_id=partner, device_id_type=MESH,
        )

    def all_sent(p):
        rows = row_of(p, 0) + (chips - 1) * unit + len(messages_of(plan[p])) * SPARE
        pltpu.make_async_remote_copy(
            src_ref=sent.at[p, pl.ds(0, rows)], dst_ref=got.at[p, pl.ds(0, rows)],
            send_sem=data_send.at[p], recv_sem=data_recv.at[p, 0],
            device_id=partner, device_id_type=MESH,
        ).wait_send()

    def multiply_all(first, last, low, high):
        def one(t, carry):
            for u in range(4):
                multiply(rows_of(plan[0], first + t * 4 + u), low, high)
            return carry

        lax.fori_loop(0, (last - first) // 4, one, 0)

    def pack(p, m, i):
        level, _, first, _, _ = messages_of(plan[p])[m]
        if level:
            value = current(p, first + i) + arrived(p, level - 1, first + i)
        else:
            value = product(p, rows_of(plan[p], first + i))
        top = jnp.max(jnp.abs(value), axis=0, keepdims=True)
        scale = TOP / jnp.maximum(top, 2e-34)
        packed = jnp.round(value * scale).astype(jnp.int32).astype(jnp.int16)
        sent[p, block_of(p, m, i), :] = packed
        sent_top[p, m, pl.ds(i, 1), :] = top

    def send(p, level):
        for m, (at, _, _, count, _) in reversed(list(enumerate(messages_of(plan[p])))):
            if at == level:
                repeat(0, count, functools.partial(pack, p, m))
                start_run(p, m, 0, count)
                start_top(p, m)

    def send_first(p, group, low=0, high=None):
        for m, (at, _, first, count, _) in enumerate(messages_of(plan[p])):
            if at:
                continue
            chunk = [i for i in range(count) if crossing(p, first + i) == 1 - group]
            ends_here = group == 1 or len(chunk) == count
            chunk = chunk[low:high]
            for i in chunk:
                pack(p, m, i)
            runs = []
            for i in chunk:
                if runs and runs[-1][1] == i:
                    runs[-1][1] = i + 1
                else:
                    runs.append([i, i + 1])
            for run in runs:
                start_run(p, m, *run)
            if chunk and ends_here and (high is None or high >= count):
                start_top(p, m)

    def remaining(p, level):
        count = [n for at, _, _, n, _ in messages_of(plan[p]) if at == level][0]
        return count

    def fill(p):
        def one(i):
            s = rows_of(plan[p], i)
            total[block_at(s), columns(p)] = product(p, s)

        repeat(0, remaining(p, 0), one)

    def wait(p, level):
        for m, (at, *_) in enumerate(messages_of(plan[p])):
            if at == level:
                whole(p, m).wait_recv()

    def keep(p, level):
        count = remaining(p, level)
        if level + 1 < len(plan[p]):
            count >>= len(plan[p][level + 1])

        def add(i):
            total[block_at(rows_of(plan[p], i)), columns(p)] += arrived(p, level, i)

        repeat(0, count, add)

    def cuts(p, side):
        q = parts - 1 - p if side == 0 else parts + p
        result = []
        for k in range(1, reach):
            for half in range(2):
                base = k * unit + (unit - tall) * half
                low, high = max(base, q * LANES), min(base + tall, (q + 1) * LANES)
                if low < high:
                    result.append((k, half, low - q * LANES, low - base, high - low))
        return result

    def flips(p, side):
        for k, half, here, there, count in cuts(p, side):
            g, m = holder(lax.rem(own + k, chips))
            yield pltpu.make_async_remote_copy(
                src_ref=flipped.at[pl.ds(p * LANES + here, count)],
                dst_ref=mirror.at[pl.ds((k - 1) * tall + there, count)],
                send_sem=flip_send, recv_sem=flip_recv,
                device_id=(g + half, m), device_id_type=MESH,
            )

    def flips_like(ref, count):
        run = pl.ds(0, count)
        return pltpu.make_async_remote_copy(
            src_ref=ref.at[run], dst_ref=ref.at[run], send_sem=flip_send, recv_sem=flip_recv,
            device_id=partner, device_id_type=MESH,
        )

    def ends(p):
        q = panel_of(p)
        at = pl.ds(pl.multiple_of(q * LANES, LANES), LANES)
        return pltpu.make_async_remote_copy(
            src_ref=last.at[p], dst_ref=window.at[:, at],
            send_sem=end_send, recv_sem=end_recv,
            device_id=partner, device_id_type=MESH,
        )

    def all_ends():
        at = pl.ds(pl.multiple_of((1 - core) * parts * LANES, LANES), parts * LANES)
        return pltpu.make_async_remote_copy(
            src_ref=window.at[:, at], dst_ref=window.at[:, at],
            send_sem=end_send, recv_sem=end_recv,
            device_id=partner, device_id_type=MESH,
        )

    def finish(p):
        mine = pl.ds(pl.multiple_of(own * unit + core * own_rows, 8), own_rows)
        theirs = pl.ds(pl.multiple_of(own * unit + (1 - core) * own_rows, 8), own_rows)
        last[p] = total[theirs, columns(p)]
        ends(p).start()
        if cuts(p, 0) or cuts(p, 1):
            value = total[block_at(own), columns(p)]
            top = jnp.max(jnp.abs(value), axis=0, keepdims=True)
            code = jnp.ceil(jnp.log2(jnp.maximum(top, 2e-34)) * CODE) + 1.0
            scale = TOP * jnp.exp2(code * (-1.0 / CODE))
            code = jnp.broadcast_to(code, (LANES - unit, LANES))
            value = jnp.concatenate([jnp.round(value * scale), code], axis=0).T
            flipped[p * LANES : (p + 1) * LANES, :] = value.astype(jnp.int32).astype(jnp.int16)
        for side in range(2):
            if cuts(p, side):
                @pl.when(core == side)
                def _():
                    for copy in flips(p, side):
                        copy.start()
        at = pl.ds(pl.multiple_of(panel_of(p) * LANES, LANES), LANES)
        window[:, at] = total[mine, columns(p)]

    early = depth // LANES * LANES
    with jax.named_scope("turn"):
        turn(0, early)
    later = chips - BEGIN
    with jax.named_scope("begin"):
        multiply_all(later, chips, 0, early)
    done = 0
    for low in range(early, 2 * depth, LANES):
        while done < pieces and low + LANES > depth + done * piece:
            with jax.named_scope(f"pair{done}"):
                pair[done].wait_recv()
            done += 1
        with jax.named_scope(f"turn{low}"):
            if low + LANES > depth:
                rows = slice(max(low, depth), low + LANES)
                both[rows, basis:] = both[rows, : parts * LANES]
            turn(low, low + LANES)
    half = (chips + later) // 2
    with jax.named_scope("multiply"):
        multiply_all(later, half, early, 2 * depth)
    with jax.named_scope("send0_0"):
        send_first(0, 0, 0, half - later)
    with jax.named_scope("multiply2"):
        multiply_all(half, chips, early, 2 * depth)
    with jax.named_scope("send1_0a"):
        send_first(1, 0)
    with jax.named_scope("send0_0b"):
        send_first(0, 0, half - later, chips)
    level = [0] * parts
    filled = [False] * parts
    for word in STARTS + [str(p) for p in ROUNDS + list(range(parts)) * 8]:
        if word[0] == "r":
            with jax.named_scope("rest" + word[1]):
                for i in range(later):
                    if crossing(0, i, ("mem", 2)) == int(word[1]):
                        multiply(rows_of(plan[0], i), 0, 2 * depth)
            continue
        p = int(word[-1])
        if p >= parts or level[p] >= len(plan[p]):
            continue
        if word[0] in "ab":
            with jax.named_scope(f"send{word}"):
                send_first(p, "ab".index(word[0]))
            continue
        if not filled[p]:
            with jax.named_scope(f"fill{p}"):
                fill(p)
            filled[p] = True
        if word[0] == "f":
            continue
        with jax.named_scope(f"wait{p}_{level[p]}"):
            wait(p, level[p])
        if level[p] + 1 < len(plan[p]):
            with jax.named_scope(f"send{p}_{level[p] + 1}"):
                send(p, level[p] + 1)
        with jax.named_scope(f"keep{p}_{level[p]}"):
            keep(p, level[p])
        level[p] += 1
        if level[p] == len(plan[p]):
            with jax.named_scope(f"finish{p}"):
                finish(p)

    with jax.named_scope("ends"):
        all_ends().wait_recv()
    for k in range(reach + 1):
        n, a = k * unit // LANES, k * unit % LANES
        value = window[:, columns(n)]
        if a:
            if a + unit > LANES:
                value = jnp.where(lane >= a, value, window[:, columns(n + 1)])
            value = pltpu.roll(value, LANES - a, 1)
        around[k] = value
    with jax.named_scope("flips"):
        flips_like(mirror, (reach - 1) * tall).wait_recv()
    for k in range(1, reach):
        low = (k - 1) * tall
        value = mirror[low : low + tall, :].astype(jnp.int32).astype(jnp.float32)
        value = jnp.where(core == 0, value[:own_rows], value[tall - own_rows :])
        scale = jnp.exp2(value[:, unit : unit + 1] * (1.0 / CODE)) * (1.0 / TOP)
        around[chips - k] = value * scale
    with jax.named_scope("out"):
      for n in range(panels):
        value, c = None, n * LANES
        while c < (n + 1) * LANES:
            b, off = c // own_rows, c % own_rows
            g, m = b // members, b % members
            s = next(s for s in range(chips) if place_of(groups, members, s) == (g // 2, m // 2, m % 2))
            piece = around[lax.rem(s - own + chips, chips)]
            shift = (c - n * LANES - (g % 2 * own_rows + off)) % LANES
            piece = pltpu.roll(piece, shift, 1) if shift else piece
            value = piece if value is None else jnp.where(lane >= c - n * LANES, piece, value)
            c += min(own_rows - off, (n + 1) * LANES - c)
        out_ref[:, columns(n)] = value
    with jax.named_scope("sents"):
        for copy in pair:
            copy.wait_send()
        for p in range(parts):
            all_sent(p)
        for side in range(2):
            count = sum(cut[4] for p in range(parts) for cut in cuts(p, side))
            pl.when(core == side)(flips_like(flipped, count).wait_send)
        all_ends().wait_send()


def circle_call(groups, members, rows, screen, own_rows, width):
    depth, basis = rows.shape
    unit = 2 * own_rows
    chips = groups * members // 2
    parts = -(-(chips // 2 + 1) * unit // LANES) // 2
    plan = circle_plan(groups, members, parts)
    levels = max(len(messages_of(stages)) for stages in plan)
    places = SPARE // 2
    deep = (chips - 1) * unit + levels * SPARE
    tall = (own_rows + 15) // 16 * 16
    pieces = PIECES
    dma = pltpu.SemaphoreType.DMA
    vmem = pl.BlockSpec(memory_space=pltpu.VMEM)
    return pl.pallas_call(
        functools.partial(circle_kernel, groups, members, plan, width),
        out_shape=pltpu.VMEM((own_rows, basis), jnp.float32),
        in_specs=[pl.BlockSpec(memory_space=pl.ANY), pl.BlockSpec(memory_space=pltpu.SMEM)],
        out_specs=vmem,
        scratch_shapes=[
            pltpu.VMEM((depth, basis), jnp.bfloat16),
            pltpu.VMEM((2 * depth, basis + parts * LANES), jnp.bfloat16),
            pltpu.VMEM((basis, 2 * depth), jnp.bfloat16),
            pltpu.VMEM((basis, (parts + 1) * LANES), jnp.float32),
            pltpu.VMEM((basis, parts * LANES), jnp.float32),
            pltpu.VMEM((parts, deep, LANES), jnp.int16),
            pltpu.VMEM((parts, deep, LANES), jnp.int16),
            pltpu.VMEM((parts, levels, places, LANES), jnp.float32),
            pltpu.VMEM((parts, levels, places, LANES), jnp.float32),
            pltpu.VMEM((parts, own_rows, LANES), jnp.float32),
            pltpu.VMEM((own_rows, 2 * parts * LANES), jnp.float32),
            pltpu.VMEM((parts * LANES, LANES), jnp.int16),
            pltpu.VMEM(((chips // 2 - 1) * tall, LANES), jnp.int16),
            pltpu.VMEM((chips, own_rows, LANES), jnp.float32),
            dma((pieces,)), dma((pieces,)), dma((pieces,)),
            dma((parts,)), dma((parts, levels)), dma, dma, dma, dma,
        ],
        compiler_params=pltpu.CompilerParams(
            collective_id=1, has_side_effects=True, vmem_limit_bytes=60 * 1024 * 1024
        ),
    )(rows, screen)


def circle_fits(groups, members, own_rows, basis, depth, width):
    unit = 2 * own_rows
    chips = groups * members // 2
    panels = -(-(chips // 2 + 1) * unit // LANES)
    return (
        groups >= 4 and members >= 4 and 64 < unit < LANES and unit % 16 == 0
        and chips // 2 <= SPARE // 2
        and basis % 256 == 0 and panels % 2 == 0 and depth % (PIECES * width) == 0
    )


def solution(mesh):
    groups, members = mesh.shape["grp"], mesh.shape["mem"]

    def on_device(factors, screen):
        aux_rows, occ_count, basis = factors.shape
        depth = aux_rows * occ_count
        devices = groups * members
        real_rows = basis // devices
        own_rows = (real_rows + 7) // 8 * 8
        rows = factors.reshape(depth, basis)
        if own_rows != real_rows:
            rows = rows.reshape(depth, devices, real_rows)
            rows = jnp.pad(rows, ((0, 0), (0, 0), (0, own_rows - real_rows)))
            basis = devices * own_rows
            rows = rows.reshape(depth, basis)
        width = occ_count // screen.shape[1]
        if own_rows == real_rows and circle_fits(groups, members, own_rows, basis, depth, width):
            return circle_call(groups, members, rows, screen, own_rows, width)
        half = basis // 2
        parts = half // LANES
        plan = plan_for(groups, members, parts)
        chunks = [(low, min(low + 2 * LANES, half)) for low in range(0, half, 2 * LANES)]
        chips = groups * members // 2
        levels = max(len(messages_of(stages)) for stages in plan)
        block = 2 * own_rows
        places = max(8, chips // 2)
        dma = pltpu.SemaphoreType.DMA
        vmem = pl.BlockSpec(memory_space=pltpu.VMEM)
        result = pl.pallas_call(
            functools.partial(kernel, groups, members, plan, chunks, occ_count // screen.shape[1]),
            out_shape=pltpu.VMEM((own_rows, basis), jnp.float32),
            in_specs=[vmem, pl.BlockSpec(memory_space=pltpu.SMEM)],
            out_specs=vmem,
            scratch_shapes=[
                pltpu.VMEM((2 * depth, basis), jnp.bfloat16),
                pltpu.VMEM((basis, 2 * depth), jnp.bfloat16),
                pltpu.VMEM((basis, half), jnp.float32),
                pltpu.VMEM((parts, chips - 1, block, LANES), jnp.int16),
                pltpu.VMEM((parts, chips - 1, block, LANES), jnp.int16),
                pltpu.VMEM((parts, levels, places, LANES), jnp.float32),
                pltpu.VMEM((parts, levels, places, LANES), jnp.float32),
                pltpu.VMEM((parts, own_rows, LANES), jnp.float32),
                dma((2,)), dma((2,)),
                dma((parts, levels)), dma((parts, levels)),
                dma((parts, levels)), dma((parts, levels)),
                dma((parts,)), dma((parts,)),
            ],
            compiler_params=pltpu.CompilerParams(
                collective_id=0, has_side_effects=True, vmem_limit_bytes=60 * 1024 * 1024
            ),
        )(rows, screen)
        if own_rows != real_rows:
            result = result[:real_rows].reshape(real_rows, devices, own_rows)[:, :, :real_rows]
            result = result.reshape(real_rows, devices * real_rows)
        return result

    placed = (P(("grp", "mem"), None, None), P(("grp", "mem"), None))
    return jax.shard_map(
        on_device, mesh=mesh, in_specs=placed, out_specs=P(("grp", "mem"), None), check_vma=False
    )
```
